32 devices in a mesh: mem: 1 (over z), row: 4 (over y), col: 4 (over x), core: 2 (over core).
Axes of the slice: x: 4, y: 4, z: 1, core: 2. Of those that a mesh axis runs over, the one named last changes fastest.
The devices are a block of a 4x4x8 slice.
Arguments:
- u_init: float32 [2048, 2048], P(('mem', 'row'), ('col', 'core'))
- forcing: float32 [2048, 2048], P(('mem', 'row'), ('col', 'core'))
- loss_weight: float32 [2048, 2048], P(('mem', 'row'), ('col', 'core'))
- stencil: float32 [3, 3], replicated
- gains: float32 [32], replicated
Outputs:
- output 1: float32 [2048, 2048], P(('mem', 'row'), ('col', 'core'))
- output 2: float32 [2048, 2048], P(('mem', 'row'), ('col', 'core'))
- output 3: float32 [2048, 2048], P(('mem', 'row'), ('col', 'core'))
All inputs are finite; a program needn't handle non-finite values.
Results may differ from the reference program's by a relative error of at most 0.001.
Values sent between devices are 32-bit elements.
A program may use at most 768 MiB of HBM per device.

```python
import jax
import jax.numpy as jnp
from jax import lax

GRID = 2048
STEPS = 32
BLOCK = 8
DT = 0.01


def seg_len(num_steps):
    best_len = 1
    for cand_len in range(1, num_steps + 1):
        if num_steps % cand_len == 0 and cand_len * cand_len <= num_steps:
            best_len = cand_len
    return best_len


def blocked(cells):
    return jnp.repeat(jnp.repeat(cells, BLOCK, axis=0), BLOCK, axis=1)


def draw_stencil(stencil_key):
    key_centre, key_total, key_share = jax.random.split(stencil_key, 3)
    centre_wt = jax.random.uniform(key_centre, (), jnp.float32, 0.3, 0.5)
    total_wt = jax.random.uniform(key_total, (), jnp.float32, 0.995, 0.999)
    share_raw = jax.random.uniform(key_share, (8,), jnp.float32, 0.5, 1.5)
    side_wts = 0.05 + (total_wt - centre_wt - 0.4) * share_raw / jnp.sum(share_raw)
    return jnp.concatenate([side_wts[:4], centre_wt[None], side_wts[4:]]).reshape(3, 3)


def setup_inputs(seed: int = 0, part: int = 0) -> dict:
    part_key = jax.random.fold_in(jax.random.key(seed), part)
    key_init, key_force, key_weight = jax.random.split(part_key, 3)
    key_stencil, key_gain = jax.random.split(jax.random.key(seed + 7777), 2)
    block_shape = (GRID // BLOCK, GRID // BLOCK)
    return {
        "u_init": blocked(0.8 * jax.random.normal(key_init, block_shape, jnp.float32)),
        "forcing": blocked(0.02 * jax.random.normal(key_force, block_shape, jnp.float32)),
        "loss_weight": blocked(jax.random.normal(key_weight, block_shape, jnp.float32)),
        "stencil": draw_stencil(key_stencil),
        "gains": jax.random.normal(key_gain, (STEPS,), jnp.float32),
    }


def one_step(field_vals, force_vals, stencil, gain_val):
    total_sum = None
    for row_off in range(3):
        for col_off in range(3):
            term_val = stencil[row_off, col_off] * jnp.roll(field_vals, (1 - row_off, 1 - col_off), axis=(0, 1))
            total_sum = term_val if total_sum is None else total_sum + term_val
    return total_sum + DT * (field_vals - field_vals * field_vals * field_vals) + gain_val * force_vals


def reference(u_init, forcing, loss_weight, stencil, gains):
    seg_steps = seg_len(STEPS)
    gain_rows = gains.reshape(STEPS // seg_steps, seg_steps)

    def run_forward(field_start, force_in):
        def segment(field_state, gain_row):
            def step_body(inner_state, gain_val):
                return one_step(inner_state, force_in, stencil, gain_val), None
            end_state, _ = lax.scan(step_body, field_state, gain_row)
            return end_state
        segment_ck = jax.checkpoint(segment)

        def outer_body(field_state, gain_row):
            return segment_ck(field_state, gain_row), None
        final_state, _ = lax.scan(outer_body, field_start, gain_rows)
        return final_state

    u_final, pullback = jax.vjp(run_forward, u_init, forcing)
    grad_init, grad_forcing = pullback(loss_weight)
    return u_final, grad_init, grad_forcing
```

```python
import functools

import jax
import jax.numpy as jnp
from jax import lax
from jax.experimental import pallas as pl
from jax.experimental.pallas import tpu as pltpu
from jax.sharding import PartitionSpec as P


DT = 0.01
LANES = 128
PHASE = 8
UNROLL = 8
MESH = pl.DeviceIdType.MESH


def stencil_blocks(load, wts, centre, nb):
    part = {}
    for b in range(nb):
        left, mid, right = load(b, -1), load(b, 0), load(b, 1)
        part[b, -1] = (wts[0][0] * left + wts[0][1] * mid) + wts[0][2] * right
        part[b, 0] = (wts[1][0] * left + centre(b, mid) * mid) + wts[1][2] * right
        part[b, 1] = (wts[2][0] * left + wts[2][1] * mid) + wts[2][2] * right
    part[-1, -1] = pltpu.roll(part[nb - 1, -1], 1, 1)
    part[nb, 1] = pltpu.roll(part[0, 1], LANES - 1, 1)
    return [(part[b - 1, -1] + part[b, 0]) + part[b + 1, 1] for b in range(nb)]


def kernel(row_size, col_size, core_size, tiles, wts_ref, gains_ref, u_hbm, f_hbm, w_hbm, uo_hbm, go_hbm, gf_hbm,
           nat, ring, lam, coef, force, acc, loc_sem, row_send, row_recv, f_send, f_recv,
           u_send, u_recv, l_send, l_recv, out_sem):
    rows, width, steps = tiles
    nb = force.shape[0]
    halo = (nb * LANES - rows) // 2
    half = halo // 2
    fdep, adep = 2 * PHASE, PHASE
    org = fdep
    phases = steps // PHASE
    groups = width // 8
    scale = DT ** 0.5

    row_id, col_id, core_id = lax.axis_index("row"), lax.axis_index("col"), lax.axis_index("core")
    up, down = lax.rem(row_id + row_size - 1, row_size), lax.rem(row_id + 1, row_size)
    flat = col_id * core_size + core_id
    total = col_size * core_size
    lflat, rflat = lax.rem(flat + total - 1, total), lax.rem(flat + 1, total)
    above, below = {"row": up}, {"row": down}
    left = {"col": lax.div(lflat, core_size), "core": lax.rem(lflat, core_size)}
    right = {"col": lax.div(rflat, core_size), "core": lax.rem(rflat, core_size)}

    srcs = (u_hbm, f_hbm, w_hbm)
    cblocks = width // LANES
    local = [[pltpu.make_async_copy(srcs[k].at[:, pl.ds(cb * LANES, LANES)], nat.at[k, cb, pl.ds(halo, rows), :],
                                    loc_sem.at[k, cb]) for cb in range(cblocks)] for k in range(3)]
    for k in range(2):
        for copy in local[k]:
            copy.start()

    barrier = pltpu.get_barrier_semaphore()
    for dev in (above, below, left, right):
        pl.semaphore_signal(barrier, inc=1, device_id=dev, device_id_type=MESH)
    pl.semaphore_wait(barrier, 4)

    def row_copies(k):
        dep = halo if k < 2 else half
        out = []
        for cb in range(cblocks):
            lanes = pl.ds(cb * LANES, LANES)
            out.append(pltpu.make_async_remote_copy(
                srcs[k].at[pl.ds(0, dep), lanes], nat.at[k, cb, pl.ds(halo + rows, dep), :],
                row_send.at[k, cb, 0], row_recv.at[k, cb, 0], device_id=above, device_id_type=MESH))
            out.append(pltpu.make_async_remote_copy(
                srcs[k].at[pl.ds(rows - dep, dep), lanes], nat.at[k, cb, pl.ds(halo - dep, dep), :],
                row_send.at[k, cb, 1], row_recv.at[k, cb, 1], device_id=below, device_id_type=MESH))
        return out

    def col_copies(ref, dep, send, recv):
        return [
            pltpu.make_async_remote_copy(ref.at[:, pl.ds(org, dep), :], ref.at[:, pl.ds(org + width, dep), :],
                                         send.at[0], recv.at[0], device_id=left, device_id_type=MESH),
            pltpu.make_async_remote_copy(ref.at[:, pl.ds(org + width - dep, dep), :], ref.at[:, pl.ds(org - dep, dep), :],
                                         send.at[1], recv.at[1], device_id=right, device_id_type=MESH),
        ]

    rcopies = [row_copies(k) for k in range(3)]
    for k in range(2):
        for copy in rcopies[k]:
            copy.start()
    for copy in local[2]:
        copy.start()
    for copy in rcopies[2]:
        copy.start()

    def arrive(k, dst, factor):
        for copy in local[k]:
            copy.wait()
        for copy in rcopies[k]:
            copy.wait()
        for cb in range(cblocks):
            for b in range(nb):
                val = jnp.transpose(nat[k, cb, pl.ds(b, LANES, stride=nb), :])
                if factor is not None:
                    val = val * factor
                dst[b, pl.ds(org + cb * LANES, LANES), :] = val

    def depart(src, k, out, factor):
        for cb in range(cblocks):
            for b in range(nb):
                val = jnp.transpose(src[b, pl.ds(org + cb * LANES, LANES), :])
                if factor is not None:
                    val = val * factor
                nat[k, cb, pl.ds(b, LANES, stride=nb), :] = val
        return [pltpu.make_async_copy(nat.at[k, cb, pl.ds(halo, rows), :], out.at[:, pl.ds(cb * LANES, LANES)],
                                      out_sem.at[k, cb]) for cb in range(cblocks)]

    arrive(0, ring.at[0], scale)
    for copy in col_copies(ring.at[0], fdep, u_send.at[0], u_recv.at[0]):
        copy.start()
    arrive(1, force, scale)
    fcopies = col_copies(force, fdep, f_send, f_recv)
    for copy in fcopies:
        copy.start()

    wts = [[wts_ref[i, j] for j in range(3)] for i in range(3)]
    flip = [[wts_ref[2 - i, 2 - j] for j in range(3)] for i in range(3)]
    mid_wt = wts_ref[1, 1] + DT

    def sweep(body, base, count):
        full, rest = divmod(count, UNROLL)
        if full == 1:
            body(base, 8 * UNROLL)
        elif full > 1:
            def block(i, _):
                body(base + i * (8 * UNROLL), 8 * UNROLL)
                return 0
            lax.fori_loop(0, full, block, 0)
        if rest:
            body(base + full * 8 * UNROLL, 8 * rest)

    def cover(step_body, dep):
        def middle():
            for j in range(1, PHASE + 1):
                sweep(functools.partial(step_body, j), org + j, groups - j)

        def sides():
            for j in range(1, PHASE):
                sweep(functools.partial(step_body, j), org + j - dep, dep // 8)
                sweep(functools.partial(step_body, j), org + width - 7 * j, -(-(dep + 6 * j) // 8))
            sweep(functools.partial(step_body, PHASE), org, PHASE // 8)
            sweep(functools.partial(step_body, PHASE), org + width - 7 * PHASE, 7 * PHASE // 8)
        return middle, sides

    def slot(phase, j):
        return lax.rem(phase * PHASE + j, 2 * PHASE)

    def reaction(val, t, b, at):
        sq = val * val
        weight = mid_wt - sq
        coef[t, b, at, :] = (weight - sq) - sq
        return weight

    def fwd_phase(phase, _):
        def step_body(j, base, cols):
            src, dst, t = slot(phase, j - 1), slot(phase, j), phase * PHASE + (j - 1)
            gain = gains_ref[t]
            at = pl.ds(base, cols)

            def centre(b, mid):
                return reaction(mid, t, b, at)
            sums = stencil_blocks(lambda b, d: ring[src, b, pl.ds(base + d, cols), :], wts, centre, nb)
            for b in range(nb):
                ring[dst, b, at, :] = sums[b] + gain * force[b, at, :]

        par = lax.rem(phase, 2)
        middle, sides = cover(step_body, fdep)
        middle()
        for copy in col_copies(ring.at[slot(phase, 0)], fdep, u_send.at[par], u_recv.at[par]):
            copy.wait()

        @pl.when(phase == 0)
        def _():
            for copy in fcopies:
                copy.wait()
        sides()
        last = phase * PHASE + (PHASE - 1)
        for at in (pl.ds(org - PHASE, PHASE), pl.ds(org + width, PHASE)):
            for b in range(nb):
                reaction(ring[slot(phase, PHASE - 1), b, at, :], last, b, at)

        @pl.when(phase < phases - 1)
        def _():
            for copy in col_copies(ring.at[slot(phase, PHASE)], fdep, u_send.at[1 - par], u_recv.at[1 - par]):
                copy.start()
        return 0

    lax.fori_loop(0, phases, fwd_phase, 0)

    arrive(2, lam.at[0], None)
    for copy in col_copies(lam.at[0], adep, l_send.at[0], l_recv.at[0]):
        copy.start()
    ucopies = depart(ring.at[(phases % 2) * PHASE], 0, uo_hbm, 1.0 / scale)
    for copy in ucopies:
        copy.start()
    acc[...] = jnp.zeros_like(acc)

    def adj_phase(phase, _):
        def step_body(j, base, cols):
            src, dst, t = slot(phase, j - 1), slot(phase, j), steps - (phase * PHASE + j)
            gain = gains_ref[t]
            at = pl.ds(base, cols)

            def centre(b, mid):
                acc[b, at, :] += gain * mid
                return coef[t, b, at, :]
            sums = stencil_blocks(lambda b, d: lam[src, b, pl.ds(base + d, cols), :], flip, centre, nb)
            for b in range(nb):
                lam[dst, b, at, :] = sums[b]

        par = lax.rem(phase, 2)
        middle, sides = cover(step_body, adep)
        middle()
        for copy in col_copies(lam.at[slot(phase, 0)], adep, l_send.at[par], l_recv.at[par]):
            copy.wait()
        sides()

        @pl.when(phase < phases - 1)
        def _():
            for copy in col_copies(lam.at[slot(phase, PHASE)], adep, l_send.at[1 - par], l_recv.at[1 - par]):
                copy.start()
        return 0

    lax.fori_loop(0, phases, adj_phase, 0)

    gcopies = depart(lam.at[(phases % 2) * PHASE], 1, go_hbm, None)
    for copy in gcopies:
        copy.start()
    fo_copies = depart(acc, 2, gf_hbm, None)
    for copy in fo_copies:
        copy.start()
    for copy in ucopies + gcopies + fo_copies:
        copy.wait()


def solution(mesh):
    row_size, col_size, core_size = mesh.shape["row"], mesh.shape["col"], mesh.shape["core"]
    field_spec = P(("mem", "row"), ("col", "core"))

    def local_run(u_init, forcing, loss_weight, weights, gains):
        rows, width = u_init.shape
        steps = gains.shape[0]
        nb = -(-(rows + 4 * steps) // LANES)
        cols = width + 4 * PHASE + 8
        cblocks = width // LANES
        f32 = jnp.float32
        field = (nb, cols, LANES)
        dma = pltpu.SemaphoreType.DMA
        hbm, smem = pl.BlockSpec(memory_space=pl.ANY), pl.BlockSpec(memory_space=pltpu.SMEM)
        return pl.pallas_call(
            functools.partial(kernel, row_size, col_size, core_size, (rows, width, steps)),
            out_shape=[jax.ShapeDtypeStruct((rows, width), f32)] * 3,
            in_specs=[smem, smem, hbm, hbm, hbm],
            out_specs=[hbm, hbm, hbm],
            scratch_shapes=[
                pltpu.VMEM((3, cblocks, nb * LANES, LANES), f32),
                pltpu.VMEM((2 * PHASE,) + field, f32),
                pltpu.VMEM((2 * PHASE,) + field, f32),
                pltpu.VMEM((steps,) + field, f32),
                pltpu.VMEM(field, f32),
                pltpu.VMEM(field, f32),
                dma((3, cblocks)),
                dma((3, cblocks, 2)),
                dma((3, cblocks, 2)),
                dma((2,)),
                dma((2,)),
                dma((2, 2)),
                dma((2, 2)),
                dma((2, 2)),
                dma((2, 2)),
                dma((3, cblocks)),
            ],
            compiler_params=pltpu.CompilerParams(
                collective_id=0, has_side_effects=True, vmem_limit_bytes=60 * 1024 * 1024),
            name="steps",
        )(weights, gains, u_init, forcing, loss_weight)

    return jax.shard_map(local_run, mesh=mesh, in_specs=(field_spec, field_spec, field_spec, P(), P()),
                         out_specs=(field_spec, field_spec, field_spec), check_vma=False)
```

```python
import functools

import jax
import jax.numpy as jnp
from jax import lax
from jax.experimental import pallas as pl
from jax.experimental.pallas import tpu as pltpu
from jax.sharding import PartitionSpec as P


DT = 0.01
LANES = 128
PHASE = 8
UNROLL = 8
MESH = pl.DeviceIdType.MESH


def stencil_blocks(load, wts, centre, nb):
    part = {}
    for b in range(nb):
        left, mid, right = load(b, -1), load(b, 0), load(b, 1)
        part[b, -1] = (wts[0][0] * left + wts[0][1] * mid) + wts[0][2] * right
        part[b, 0] = (wts[1][0] * left + centre(b, mid) * mid) + wts[1][2] * right
        part[b, 1] = (wts[2][0] * left + wts[2][1] * mid) + wts[2][2] * right
    part[-1, -1] = pltpu.roll(part[nb - 1, -1], 1, 1)
    part[nb, 1] = pltpu.roll(part[0, 1], LANES - 1, 1)
    return [(part[b - 1, -1] + part[b, 0]) + part[b + 1, 1] for b in range(nb)]


def kernel(row_size, col_size, core_size, tiles, wts_ref, gains_ref, u_hbm, f_hbm, w_hbm, uo_hbm, go_hbm, gf_hbm,
           nat, ubase, lbase, inner, coef, force, acc, loc_sem, row_send, row_recv, f_send, f_recv,
           u_send, u_recv, l_send, l_recv, out_sem):
    rows, width, steps = tiles
    nb = force.shape[0]
    halo = (nb * LANES - rows) // 2
    half = halo // 2
    fdep, adep = 2 * PHASE, PHASE
    org = fdep
    phases = steps // PHASE
    groups = width // 8
    scale = DT ** 0.5

    row_id, col_id, core_id = lax.axis_index("row"), lax.axis_index("col"), lax.axis_index("core")
    up, down = lax.rem(row_id + row_size - 1, row_size), lax.rem(row_id + 1, row_size)
    flat = col_id * core_size + core_id
    total = col_size * core_size
    lflat, rflat = lax.rem(flat + total - 1, total), lax.rem(flat + 1, total)
    above, below = {"row": up}, {"row": down}
    left = {"col": lax.div(lflat, core_size), "core": lax.rem(lflat, core_size)}
    right = {"col": lax.div(rflat, core_size), "core": lax.rem(rflat, core_size)}

    srcs = (u_hbm, f_hbm, w_hbm)
    cblocks = width // LANES
    local = [[pltpu.make_async_copy(srcs[k].at[:, pl.ds(cb * LANES, LANES)], nat.at[k, cb, pl.ds(halo, rows), :],
                                    loc_sem.at[k, cb]) for cb in range(cblocks)] for k in range(3)]
    for k in range(2):
        for copy in local[k]:
            copy.start()

    barrier = pltpu.get_barrier_semaphore()
    for dev in (above, below, left, right):
        pl.semaphore_signal(barrier, inc=1, device_id=dev, device_id_type=MESH)
    pl.semaphore_wait(barrier, 4)

    def row_copies(k):
        dep = halo if k < 2 else half
        out = []
        for cb in range(cblocks):
            lanes = pl.ds(cb * LANES, LANES)
            out.append(pltpu.make_async_remote_copy(
                srcs[k].at[pl.ds(0, dep), lanes], nat.at[k, cb, pl.ds(halo + rows, dep), :],
                row_send.at[k, cb, 0], row_recv.at[k, cb, 0], device_id=above, device_id_type=MESH))
            out.append(pltpu.make_async_remote_copy(
                srcs[k].at[pl.ds(rows - dep, dep), lanes], nat.at[k, cb, pl.ds(halo - dep, dep), :],
                row_send.at[k, cb, 1], row_recv.at[k, cb, 1], device_id=below, device_id_type=MESH))
        return out

    def col_copies(ref, dep, send, recv):
        return [
            pltpu.make_async_remote_copy(ref.at[:, pl.ds(org, dep), :], ref.at[:, pl.ds(org + width, dep), :],
                                         send.at[0], recv.at[0], device_id=left, device_id_type=MESH),
            pltpu.make_async_remote_copy(ref.at[:, pl.ds(org + width - dep, dep), :], ref.at[:, pl.ds(org - dep, dep), :],
                                         send.at[1], recv.at[1], device_id=right, device_id_type=MESH),
        ]

    rcopies = [row_copies(k) for k in range(3)]
    for k in range(2):
        for copy in rcopies[k]:
            copy.start()
    for copy in local[2]:
        copy.start()
    for copy in rcopies[2]:
        copy.start()

    def arrive(k, dst, factor):
        for copy in local[k]:
            copy.wait()
        for copy in rcopies[k]:
            copy.wait()
        for cb in range(cblocks):
            for b in range(nb):
                val = jnp.transpose(nat[k, cb, pl.ds(b, LANES, stride=nb), :])
                if factor is not None:
                    val = val * factor
                dst[b, pl.ds(org + cb * LANES, LANES), :] = val

    def depart(src, k, out, factor):
        for cb in range(cblocks):
            for b in range(nb):
                val = jnp.transpose(src[b, pl.ds(org + cb * LANES, LANES), :])
                if factor is not None:
                    val = val * factor
                nat[k, cb, pl.ds(b, LANES, stride=nb), :] = val
        return [pltpu.make_async_copy(nat.at[k, cb, pl.ds(halo, rows), :], out.at[:, pl.ds(cb * LANES, LANES)],
                                      out_sem.at[k, cb]) for cb in range(cblocks)]

    arrive(0, ubase.at[0], scale)
    for copy in col_copies(ubase.at[0], fdep, u_send.at[0], u_recv.at[0]):
        copy.start()
    arrive(1, force, scale)
    fcopies = col_copies(force, fdep, f_send, f_recv)
    for copy in fcopies:
        copy.start()

    wts = [[wts_ref[i, j] for j in range(3)] for i in range(3)]
    flip = [[wts_ref[2 - i, 2 - j] for j in range(3)] for i in range(3)]
    mid_wt = wts_ref[1, 1] + DT

    def sweep(body, base, count):
        full, rest = divmod(count, UNROLL)
        if full == 1:
            body(base, 8 * UNROLL)
        elif full > 1:
            def block(i, _):
                body(base + i * (8 * UNROLL), 8 * UNROLL)
                return 0
            lax.fori_loop(0, full, block, 0)
        if rest:
            body(base + full * 8 * UNROLL, 8 * rest)

    def cover(step_body, dep):
        def middle():
            for j in range(1, PHASE + 1):
                sweep(functools.partial(step_body, j), org + j, groups - j)

        def sides():
            for j in range(1, PHASE):
                sweep(functools.partial(step_body, j), org + j - dep, dep // 8)
                sweep(functools.partial(step_body, j), org + width - 7 * j, -(-(dep + 6 * j) // 8))
            sweep(functools.partial(step_body, PHASE), org, PHASE // 8)
            sweep(functools.partial(step_body, PHASE), org + width - 7 * PHASE, 7 * PHASE // 8)
        return middle, sides

    def level(base, par, j):
        if j == 0:
            return base.at[par]
        return base.at[1 - par] if j == PHASE else inner.at[j - 1]

    def reaction(val, t, b, at):
        sq = val * val
        weight = mid_wt - sq
        coef[t, b, at, :] = (weight - sq) - sq
        return weight

    def fwd_phase(phase, _):
        par = lax.rem(phase, 2)

        def step_body(j, base, cols):
            src, dst, t = level(ubase, par, j - 1), level(ubase, par, j), phase * PHASE + (j - 1)
            gain = gains_ref[t]
            at = pl.ds(base, cols)

            def centre(b, mid):
                return reaction(mid, t, b, at)
            sums = stencil_blocks(lambda b, d: src[b, pl.ds(base + d, cols), :], wts, centre, nb)
            for b in range(nb):
                dst[b, at, :] = sums[b] + gain * force[b, at, :]

        middle, sides = cover(step_body, fdep)
        middle()
        for copy in col_copies(ubase.at[par], fdep, u_send.at[par], u_recv.at[par]):
            copy.wait()

        @pl.when(phase == 0)
        def _():
            for copy in fcopies:
                copy.wait()
        sides()
        last = phase * PHASE + (PHASE - 1)
        for at in (pl.ds(org - PHASE, PHASE), pl.ds(org + width, PHASE)):
            for b in range(nb):
                reaction(inner[PHASE - 2, b, at, :], last, b, at)

        @pl.when(phase < phases - 1)
        def _():
            for copy in col_copies(ubase.at[1 - par], fdep, u_send.at[1 - par], u_recv.at[1 - par]):
                copy.start()
        return 0

    lax.fori_loop(0, phases, fwd_phase, 0)

    arrive(2, lbase.at[0], None)
    for copy in col_copies(lbase.at[0], adep, l_send.at[0], l_recv.at[0]):
        copy.start()
    ucopies = depart(ubase.at[phases % 2], 0, uo_hbm, 1.0 / scale)
    for copy in ucopies:
        copy.start()
    acc[...] = jnp.zeros_like(acc)

    def adj_phase(phase, _):
        par = lax.rem(phase, 2)

        def step_body(j, base, cols):
            src, dst, t = level(lbase, par, j - 1), level(lbase, par, j), steps - (phase * PHASE + j)
            gain = gains_ref[t]
            at = pl.ds(base, cols)

            def centre(b, mid):
                acc[b, at, :] += gain * mid
                return coef[t, b, at, :]
            sums = stencil_blocks(lambda b, d: src[b, pl.ds(base + d, cols), :], flip, centre, nb)
            for b in range(nb):
                dst[b, at, :] = sums[b]

        middle, sides = cover(step_body, adep)
        middle()
        for copy in col_copies(lbase.at[par], adep, l_send.at[par], l_recv.at[par]):
            copy.wait()
        sides()

        @pl.when(phase < phases - 1)
        def _():
            for copy in col_copies(lbase.at[1 - par], adep, l_send.at[1 - par], l_recv.at[1 - par]):
                copy.start()
        return 0

    lax.fori_loop(0, phases, adj_phase, 0)

    gcopies = depart(lbase.at[phases % 2], 1, go_hbm, None)
    for copy in gcopies:
        copy.start()
    fo_copies = depart(acc, 2, gf_hbm, None)
    for copy in fo_copies:
        copy.start()
    for copy in ucopies + gcopies + fo_copies:
        copy.wait()


def solution(mesh):
    row_size, col_size, core_size = mesh.shape["row"], mesh.shape["col"], mesh.shape["core"]
    field_spec = P(("mem", "row"), ("col", "core"))

    def local_run(u_init, forcing, loss_weight, weights, gains):
        rows, width = u_init.shape
        steps = gains.shape[0]
        nb = -(-(rows + 4 * steps) // LANES)
        cols = width + 4 * PHASE + 8
        cblocks = width // LANES
        f32 = jnp.float32
        field = (nb, cols, LANES)
        dma = pltpu.SemaphoreType.DMA
        hbm, smem = pl.BlockSpec(memory_space=pl.ANY), pl.BlockSpec(memory_space=pltpu.SMEM)
        return pl.pallas_call(
            functools.partial(kernel, row_size, col_size, core_size, (rows, width, steps)),
            out_shape=[jax.ShapeDtypeStruct((rows, width), f32)] * 3,
            in_specs=[smem, smem, hbm, hbm, hbm],
            out_specs=[hbm, hbm, hbm],
            scratch_shapes=[
                pltpu.VMEM((3, cblocks, nb * LANES, LANES), f32),
                pltpu.VMEM((2,) + field, f32),
                pltpu.VMEM((2,) + field, f32),
                pltpu.VMEM((PHASE - 1,) + field, f32),
                pltpu.VMEM((steps,) + field, f32),
                pltpu.VMEM(field, f32),
                pltpu.VMEM(field, f32),
                dma((3, cblocks)),
                dma((3, cblocks, 2)),
                dma((3, cblocks, 2)),
                dma((2,)),
                dma((2,)),
                dma((2, 2)),
                dma((2, 2)),
                dma((2, 2)),
                dma((2, 2)),
                dma((3, cblocks)),
            ],
            compiler_params=pltpu.CompilerParams(
                collective_id=0, has_side_effects=True, vmem_limit_bytes=60 * 1024 * 1024),
            name="steps",
        )(weights, gains, u_init, forcing, loss_weight)

    return jax.shard_map(local_run, mesh=mesh, in_specs=(field_spec, field_spec, field_spec, P(), P()),
                         out_specs=(field_spec, field_spec, field_spec), check_vma=False)
```

```python
import functools

import jax
import jax.numpy as jnp
from jax import lax
from jax.experimental import pallas as pl
from jax.experimental.pallas import tpu as pltpu
from jax.sharding import PartitionSpec as P


DT = 0.01
LANES = 128
PHASE = 8
UNROLL = 8
MESH = pl.DeviceIdType.MESH


def stencil_blocks(load, wts, centre, nb):
    part = {}
    for b in range(nb):
        left, mid, right = load(b, -1), load(b, 0), load(b, 1)
        part[b, -1] = (wts[0][0] * left + wts[0][1] * mid) + wts[0][2] * right
        part[b, 0] = (wts[1][0] * left + centre(b, mid) * mid) + wts[1][2] * right
        part[b, 1] = (wts[2][0] * left + wts[2][1] * mid) + wts[2][2] * right
    part[-1, -1] = pltpu.roll(part[nb - 1, -1], 1, 1)
    part[nb, 1] = pltpu.roll(part[0, 1], LANES - 1, 1)
    return [(part[b - 1, -1] + part[b, 0]) + part[b + 1, 1] for b in range(nb)]


def kernel(row_size, col_size, core_size, tiles, wts_hbm, gains_hbm, u_hbm, f_hbm, w_hbm, uo_ref, go_ref, gf_ref,
           wts_ref, gains_ref, nat, ubase, lbase, inner, coef, force, acc, par_sem, loc_sem, row_send, row_recv, f_send, f_recv,
           u_send, u_recv, l_send, l_recv):
    rows, width, steps = tiles
    nb = force.shape[0]
    halo = (nb * LANES - rows) // 2
    half = halo // 2
    fdep, adep = 2 * PHASE, PHASE
    org = fdep
    phases = steps // PHASE
    groups = width // 8
    scale = DT ** 0.5

    row_id, col_id, core_id = lax.axis_index("row"), lax.axis_index("col"), lax.axis_index("core")
    up, down = lax.rem(row_id + row_size - 1, row_size), lax.rem(row_id + 1, row_size)
    flat = col_id * core_size + core_id
    total = col_size * core_size
    lflat, rflat = lax.rem(flat + total - 1, total), lax.rem(flat + 1, total)
    above, below = {"row": up}, {"row": down}
    left = {"col": lax.div(lflat, core_size), "core": lax.rem(lflat, core_size)}
    right = {"col": lax.div(rflat, core_size), "core": lax.rem(rflat, core_size)}

    srcs = (u_hbm, f_hbm, w_hbm)
    cblocks = width // LANES
    local = [[pltpu.make_async_copy(srcs[k].at[:, pl.ds(cb * LANES, LANES)], nat.at[k, cb, pl.ds(halo, rows), :],
                                    loc_sem.at[k, cb]) for cb in range(cblocks)] for k in range(3)]
    for k in range(3):
        for copy in local[k]:
            copy.start()
    params = [pltpu.make_async_copy(wts_hbm, wts_ref, par_sem.at[0]),
              pltpu.make_async_copy(gains_hbm, gains_ref, par_sem.at[1])]
    for copy in params:
        copy.start()

    barrier = pltpu.get_barrier_semaphore()
    for dev in (above, below, left, right):
        pl.semaphore_signal(barrier, inc=1, device_id=dev, device_id_type=MESH)
    pl.semaphore_wait(barrier, 4)

    def row_copies(k):
        dep = halo if k < 2 else half
        out = []
        for cb in range(cblocks):
            out.append(pltpu.make_async_remote_copy(
                nat.at[k, cb, pl.ds(halo, dep), :], nat.at[k, cb, pl.ds(halo + rows, dep), :],
                row_send.at[k, cb, 0], row_recv.at[k, cb, 0], device_id=above, device_id_type=MESH))
            out.append(pltpu.make_async_remote_copy(
                nat.at[k, cb, pl.ds(halo + rows - dep, dep), :], nat.at[k, cb, pl.ds(halo - dep, dep), :],
                row_send.at[k, cb, 1], row_recv.at[k, cb, 1], device_id=below, device_id_type=MESH))
        return out

    def col_copies(ref, dep, send, recv):
        return [
            pltpu.make_async_remote_copy(ref.at[:, pl.ds(org, dep), :], ref.at[:, pl.ds(org + width, dep), :],
                                         send.at[0], recv.at[0], device_id=left, device_id_type=MESH),
            pltpu.make_async_remote_copy(ref.at[:, pl.ds(org + width - dep, dep), :], ref.at[:, pl.ds(org - dep, dep), :],
                                         send.at[1], recv.at[1], device_id=right, device_id_type=MESH),
        ]

    rcopies = [row_copies(k) for k in range(3)]
    for k in range(3):
        for copy in local[k]:
            copy.wait()
        for copy in rcopies[k]:
            copy.start()
    for copy in params:
        copy.wait()

    def arrive(k, dst, factor):
        for copy in rcopies[k]:
            copy.wait()
        for cb in range(cblocks):
            for b in range(nb):
                val = jnp.transpose(nat[k, cb, pl.ds(b, LANES, stride=nb), :])
                if factor is not None:
                    val = val * factor
                dst[b, pl.ds(org + cb * LANES, LANES), :] = val

    def depart(src, k, out, factor):
        for cb in range(cblocks):
            for b in range(nb):
                val = jnp.transpose(src[b, pl.ds(org + cb * LANES, LANES), :])
                if factor is not None:
                    val = val * factor
                nat[k, cb, pl.ds(b, LANES, stride=nb), :] = val
            out[:, pl.ds(cb * LANES, LANES)] = nat[k, cb, pl.ds(halo, rows), :]

    arrive(0, ubase.at[0], scale)
    for copy in col_copies(ubase.at[0], fdep, u_send.at[0], u_recv.at[0]):
        copy.start()
    arrive(1, force, scale)
    fcopies = col_copies(force, fdep, f_send, f_recv)
    for copy in fcopies:
        copy.start()

    wts = [[wts_ref[i, j] for j in range(3)] for i in range(3)]
    flip = [[wts_ref[2 - i, 2 - j] for j in range(3)] for i in range(3)]
    mid_wt = wts_ref[1, 1] + DT

    def sweep(body, base, count):
        full, rest = divmod(count, UNROLL)
        if full == 1:
            body(base, 8 * UNROLL)
        elif full > 1:
            def block(i, _):
                body(base + i * (8 * UNROLL), 8 * UNROLL)
                return 0
            lax.fori_loop(0, full, block, 0)
        if rest:
            body(base + full * 8 * UNROLL, 8 * rest)

    def cover(step_body, dep):
        def middle():
            for j in range(1, PHASE + 1):
                sweep(functools.partial(step_body, j), org + j, groups - j)

        def sides():
            for j in range(1, PHASE):
                sweep(functools.partial(step_body, j), org + j - dep, dep // 8)
                sweep(functools.partial(step_body, j), org + width - 7 * j, -(-(dep + 6 * j) // 8))
            sweep(functools.partial(step_body, PHASE), org, PHASE // 8)
            sweep(functools.partial(step_body, PHASE), org + width - 7 * PHASE, 7 * PHASE // 8)
        return middle, sides

    def level(base, par, j):
        if j == 0:
            return base.at[par]
        return base.at[1 - par] if j == PHASE else inner.at[j - 1]

    def reaction(val, t, b, at):
        sq = val * val
        weight = mid_wt - sq
        coef[t, b, at, :] = (weight - sq) - sq
        return weight

    def fwd_phase(phase, _):
        par = lax.rem(phase, 2)

        def step_body(j, base, cols):
            src, dst, t = level(ubase, par, j - 1), level(ubase, par, j), phase * PHASE + (j - 1)
            gain = gains_ref[t]
            at = pl.ds(base, cols)

            def centre(b, mid):
                return reaction(mid, t, b, at)
            sums = stencil_blocks(lambda b, d: src[b, pl.ds(base + d, cols), :], wts, centre, nb)
            for b in range(nb):
                dst[b, at, :] = sums[b] + gain * force[b, at, :]

        middle, sides = cover(step_body, fdep)
        middle()
        for copy in col_copies(ubase.at[par], fdep, u_send.at[par], u_recv.at[par]):
            copy.wait()

        @pl.when(phase == 0)
        def _():
            for copy in fcopies:
                copy.wait()
        sides()
        last = phase * PHASE + (PHASE - 1)
        for at in (pl.ds(org - PHASE, PHASE), pl.ds(org + width, PHASE)):
            for b in range(nb):
                reaction(inner[PHASE - 2, b, at, :], last, b, at)

        @pl.when(phase < phases - 1)
        def _():
            for copy in col_copies(ubase.at[1 - par], fdep, u_send.at[1 - par], u_recv.at[1 - par]):
                copy.start()
        return 0

    lax.fori_loop(0, phases, fwd_phase, 0)

    arrive(2, lbase.at[0], None)
    for copy in col_copies(lbase.at[0], adep, l_send.at[0], l_recv.at[0]):
        copy.start()
    depart(ubase.at[phases % 2], 0, uo_ref, 1.0 / scale)
    acc[...] = jnp.zeros_like(acc)

    def adj_phase(phase, _):
        par = lax.rem(phase, 2)

        def step_body(j, base, cols):
            src, dst, t = level(lbase, par, j - 1), level(lbase, par, j), steps - (phase * PHASE + j)
            gain = gains_ref[t]
            at = pl.ds(base, cols)

            def centre(b, mid):
                acc[b, at, :] += gain * mid
                return coef[t, b, at, :]
            sums = stencil_blocks(lambda b, d: src[b, pl.ds(base + d, cols), :], flip, centre, nb)
            for b in range(nb):
                dst[b, at, :] = sums[b]

        middle, sides = cover(step_body, adep)
        middle()
        for copy in col_copies(lbase.at[par], adep, l_send.at[par], l_recv.at[par]):
            copy.wait()
        sides()

        @pl.when(phase < phases - 1)
        def _():
            for copy in col_copies(lbase.at[1 - par], adep, l_send.at[1 - par], l_recv.at[1 - par]):
                copy.start()
        return 0

    lax.fori_loop(0, phases, adj_phase, 0)

    depart(lbase.at[phases % 2], 1, go_ref, None)
    depart(acc, 2, gf_ref, None)


def solution(mesh):
    row_size, col_size, core_size = mesh.shape["row"], mesh.shape["col"], mesh.shape["core"]
    field_spec = P(("mem", "row"), ("col", "core"))

    def local_run(u_init, forcing, loss_weight, weights, gains):
        rows, width = u_init.shape
        steps = gains.shape[0]
        nb = -(-(rows + 4 * steps) // LANES)
        cols = width + 4 * PHASE + 8
        cblocks = width // LANES
        f32 = jnp.float32
        field = (nb, cols, LANES)
        dma = pltpu.SemaphoreType.DMA
        hbm, vmem = pl.BlockSpec(memory_space=pl.ANY), pl.BlockSpec(memory_space=pltpu.VMEM)
        return pl.pallas_call(
            functools.partial(kernel, row_size, col_size, core_size, (rows, width, steps)),
            out_shape=[jax.ShapeDtypeStruct((rows, width), f32)] * 3,
            in_specs=[hbm] * 5,
            out_specs=[vmem, vmem, vmem],
            scratch_shapes=[
                pltpu.SMEM(weights.shape, f32),
                pltpu.SMEM(gains.shape, f32),
                pltpu.VMEM((3, cblocks, nb * LANES, LANES), f32),
                pltpu.VMEM((2,) + field, f32),
                pltpu.VMEM((2,) + field, f32),
                pltpu.VMEM((PHASE - 1,) + field, f32),
                pltpu.VMEM((steps,) + field, f32),
                pltpu.VMEM(field, f32),
                pltpu.VMEM(field, f32),
                dma((2,)),
                dma((3, cblocks)),
                dma((3, cblocks, 2)),
                dma((3, cblocks, 2)),
                dma((2,)),
                dma((2,)),
                dma((2, 2)),
                dma((2, 2)),
                dma((2, 2)),
                dma((2, 2)),
            ],
            compiler_params=pltpu.CompilerParams(
                collective_id=0, has_side_effects=True, vmem_limit_bytes=48 * 1024 * 1024),
            name="steps",
        )(*(pltpu.with_memory_space_constraint(x, pltpu.HBM) for x in (weights, gains, u_init, forcing, loss_weight)))

    return jax.shard_map(local_run, mesh=mesh, in_specs=(field_spec, field_spec, field_spec, P(), P()),
                         out_specs=(field_spec, field_spec, field_spec), check_vma=False)
```

```python
import functools

import jax
import jax.numpy as jnp
from jax import lax
from jax.experimental import pallas as pl
from jax.experimental.pallas import tpu as pltpu
from jax.sharding import PartitionSpec as P


DT = 0.01
LANES = 128
PHASE = 8
APART = 4
UNROLL = 8
MESH = pl.DeviceIdType.MESH


def stencil_blocks(load, wts, centre, nb):
    part = {}
    for b in range(nb):
        left, mid, right = load(b, -1), load(b, 0), load(b, 1)
        part[b, -1] = (wts[0][0] * left + wts[0][1] * mid) + wts[0][2] * right
        part[b, 0] = (wts[1][0] * left + centre(b, mid) * mid) + wts[1][2] * right
        part[b, 1] = (wts[2][0] * left + wts[2][1] * mid) + wts[2][2] * right
    part[-1, -1] = pltpu.roll(part[nb - 1, -1], 1, 1)
    part[nb, 1] = pltpu.roll(part[0, 1], LANES - 1, 1)
    return [(part[b - 1, -1] + part[b, 0]) + part[b + 1, 1] for b in range(nb)]


def kernel(row_size, col_size, core_size, tiles, wts_hbm, gains_hbm, u_hbm, f_hbm, w_hbm, uo_ref, go_ref, gf_ref,
           wts_ref, gains_ref, nat, ubase, lbase, inner, coef, force, acc, par_sem, loc_sem, row_send, row_recv, f_send, f_recv,
           u_send, u_recv, l_send, l_recv):
    rows, width, steps = tiles
    nb = force.shape[0]
    halo = (nb * LANES - rows) // 2
    half = halo // 2
    fdep, adep = 2 * PHASE, PHASE
    org = fdep
    phases = steps // PHASE
    groups = width // 8
    scale = DT ** 0.5

    row_id, col_id, core_id = lax.axis_index("row"), lax.axis_index("col"), lax.axis_index("core")
    up, down = lax.rem(row_id + row_size - 1, row_size), lax.rem(row_id + 1, row_size)
    flat = col_id * core_size + core_id
    total = col_size * core_size
    lflat, rflat = lax.rem(flat + total - 1, total), lax.rem(flat + 1, total)
    above, below = {"row": up}, {"row": down}
    left = {"col": lax.div(lflat, core_size), "core": lax.rem(lflat, core_size)}
    right = {"col": lax.div(rflat, core_size), "core": lax.rem(rflat, core_size)}

    srcs = (u_hbm, f_hbm, w_hbm)
    cblocks = width // LANES
    local = [[pltpu.make_async_copy(srcs[k].at[:, pl.ds(cb * LANES, LANES)], nat.at[k, cb, pl.ds(halo, rows), :],
                                    loc_sem.at[k, cb]) for cb in range(cblocks)] for k in range(3)]
    for k in range(3):
        for copy in local[k]:
            copy.start()
    params = [pltpu.make_async_copy(wts_hbm, wts_ref, par_sem.at[0]),
              pltpu.make_async_copy(gains_hbm, gains_ref, par_sem.at[1])]
    for copy in params:
        copy.start()

    barrier = pltpu.get_barrier_semaphore()
    for dev in (above, below, left, right):
        pl.semaphore_signal(barrier, inc=1, device_id=dev, device_id_type=MESH)
    pl.semaphore_wait(barrier, 4)

    def row_copies(k):
        dep = halo if k < 2 else half
        out = []
        for cb in range(cblocks):
            out.append(pltpu.make_async_remote_copy(
                nat.at[k, cb, pl.ds(halo, dep), :], nat.at[k, cb, pl.ds(halo + rows, dep), :],
                row_send.at[k, cb, 0], row_recv.at[k, cb, 0], device_id=above, device_id_type=MESH))
            out.append(pltpu.make_async_remote_copy(
                nat.at[k, cb, pl.ds(halo + rows - dep, dep), :], nat.at[k, cb, pl.ds(halo - dep, dep), :],
                row_send.at[k, cb, 1], row_recv.at[k, cb, 1], device_id=below, device_id_type=MESH))
        return out

    def col_copies(ref, dep, send, recv):
        return [
            pltpu.make_async_remote_copy(ref.at[:, pl.ds(org, dep), :], ref.at[:, pl.ds(org + width, dep), :],
                                         send.at[0], recv.at[0], device_id=left, device_id_type=MESH),
            pltpu.make_async_remote_copy(ref.at[:, pl.ds(org + width - dep, dep), :], ref.at[:, pl.ds(org - dep, dep), :],
                                         send.at[1], recv.at[1], device_id=right, device_id_type=MESH),
        ]

    rcopies = [row_copies(k) for k in range(3)]
    for k in range(3):
        for copy in local[k]:
            copy.wait()
        for copy in rcopies[k]:
            copy.start()
    for copy in params:
        copy.wait()

    def arrive(k, dst, factor):
        for copy in rcopies[k]:
            copy.wait()
        for cb in range(cblocks):
            for b in range(nb):
                val = jnp.transpose(nat[k, cb, pl.ds(b, LANES, stride=nb), :])
                if factor is not None:
                    val = val * factor
                dst[b, pl.ds(org + cb * LANES, LANES), :] = val

    def depart(src, k, out, factor):
        for cb in range(cblocks):
            for b in range(nb):
                val = jnp.transpose(src[b, pl.ds(org + cb * LANES, LANES), :])
                if factor is not None:
                    val = val * factor
                nat[k, cb, pl.ds(b, LANES, stride=nb), :] = val
            out[:, pl.ds(cb * LANES, LANES)] = nat[k, cb, pl.ds(halo, rows), :]

    arrive(0, ubase.at[0], scale)
    for copy in col_copies(ubase.at[0], fdep, u_send.at[0], u_recv.at[0]):
        copy.start()
    arrive(1, force, scale)
    fcopies = col_copies(force, fdep, f_send, f_recv)
    for copy in fcopies:
        copy.start()

    wts = [[wts_ref[i, j] for j in range(3)] for i in range(3)]
    flip = [[wts_ref[2 - i, 2 - j] for j in range(3)] for i in range(3)]
    mid_wt = wts_ref[1, 1] + DT

    def sweep(body, base, count):
        for off in range(0, count, 8 * UNROLL):
            body(base + off, min(8 * UNROLL, count - off))

    def cover(step_body, dep):
        def middle():
            for j in range(1, PHASE + 1):
                sweep(functools.partial(step_body, j), org + j, width - 2 * j)

        def sides():
            for j in range(1, PHASE):
                sweep(functools.partial(step_body, j), org + j - dep, dep)
                sweep(functools.partial(step_body, j), org + width - j, dep)
            sweep(functools.partial(step_body, PHASE), org, PHASE)
            sweep(functools.partial(step_body, PHASE), org + width - PHASE, PHASE)
        return middle, sides

    def level(base, par, j):
        if j == 0:
            return base.at[par * APART]
        return base.at[(1 - par) * APART] if j == PHASE else inner.at[j - 1]

    def reaction(val, t, b, at):
        sq = val * val
        weight = mid_wt - sq
        coef[t, b, at, :] = (weight - sq) - sq
        return weight

    def fwd_phase(phase, _):
        par = lax.rem(phase, 2)

        def step_body(j, base, cols):
            src, dst, t = level(ubase, par, j - 1), level(ubase, par, j), phase * PHASE + (j - 1)
            gain = gains_ref[t]
            at = pl.ds(base, cols)

            def centre(b, mid):
                return reaction(mid, t, b, at)
            sums = stencil_blocks(lambda b, d: src[b, pl.ds(base + d, cols), :], wts, centre, nb)
            for b in range(nb):
                dst[b, at, :] = sums[b] + gain * force[b, at, :]

        middle, sides = cover(step_body, fdep)
        middle()
        for copy in col_copies(ubase.at[par * APART], fdep, u_send.at[par], u_recv.at[par]):
            copy.wait()

        @pl.when(phase == 0)
        def _():
            for copy in fcopies:
                copy.wait()
        sides()
        last = phase * PHASE + (PHASE - 1)
        for at in (pl.ds(org - PHASE, PHASE), pl.ds(org + width, PHASE)):
            for b in range(nb):
                reaction(inner[PHASE - 2, b, at, :], last, b, at)

        @pl.when(phase < phases - 1)
        def _():
            for copy in col_copies(ubase.at[(1 - par) * APART], fdep, u_send.at[1 - par], u_recv.at[1 - par]):
                copy.start()
        return 0

    lax.fori_loop(0, phases, fwd_phase, 0)

    arrive(2, lbase.at[0], None)
    for copy in col_copies(lbase.at[0], adep, l_send.at[0], l_recv.at[0]):
        copy.start()
    depart(ubase.at[phases % 2 * APART], 0, uo_ref, 1.0 / scale)
    acc[...] = jnp.zeros_like(acc)

    def adj_phase(phase, _):
        par = lax.rem(phase, 2)

        def step_body(j, base, cols):
            src, dst, t = level(lbase, par, j - 1), level(lbase, par, j), steps - (phase * PHASE + j)
            gain = gains_ref[t]
            at = pl.ds(base, cols)

            def centre(b, mid):
                acc[b, at, :] += gain * mid
                return coef[t, b, at, :]
            sums = stencil_blocks(lambda b, d: src[b, pl.ds(base + d, cols), :], flip, centre, nb)
            for b in range(nb):
                dst[b, at, :] = sums[b]

        middle, sides = cover(step_body, adep)
        middle()
        for copy in col_copies(lbase.at[par * APART], adep, l_send.at[par], l_recv.at[par]):
            copy.wait()
        sides()

        @pl.when(phase < phases - 1)
        def _():
            for copy in col_copies(lbase.at[(1 - par) * APART], adep, l_send.at[1 - par], l_recv.at[1 - par]):
                copy.start()
        return 0

    lax.fori_loop(0, phases, adj_phase, 0)

    depart(lbase.at[phases % 2 * APART], 1, go_ref, None)
    depart(acc, 2, gf_ref, None)


def solution(mesh):
    row_size, col_size, core_size = mesh.shape["row"], mesh.shape["col"], mesh.shape["core"]
    field_spec = P(("mem", "row"), ("col", "core"))

    def local_run(u_init, forcing, loss_weight, weights, gains):
        rows, width = u_init.shape
        steps = gains.shape[0]
        nb = -(-(rows + 4 * steps) // LANES)
        cols = width + 4 * PHASE + 8
        cblocks = width // LANES
        f32 = jnp.float32
        field = (nb, cols, LANES)
        dma = pltpu.SemaphoreType.DMA
        hbm, vmem = pl.BlockSpec(memory_space=pl.ANY), pl.BlockSpec(memory_space=pltpu.VMEM)
        return pl.pallas_call(
            functools.partial(kernel, row_size, col_size, core_size, (rows, width, steps)),
            out_shape=[jax.ShapeDtypeStruct((rows, width), f32)] * 3,
            in_specs=[hbm] * 5,
            out_specs=[vmem, vmem, vmem],
            scratch_shapes=[
                pltpu.SMEM(weights.shape, f32),
                pltpu.SMEM(gains.shape, f32),
                pltpu.VMEM((3, cblocks, nb * LANES, LANES), f32),
                pltpu.VMEM((1 + APART,) + field, f32),
                pltpu.VMEM((1 + APART,) + field, f32),
                pltpu.VMEM((PHASE - 1,) + field, f32),
                pltpu.VMEM((steps,) + field, f32),
                pltpu.VMEM(field, f32),
                pltpu.VMEM(field, f32),
                dma((2,)),
                dma((3, cblocks)),
                dma((3, cblocks, 2)),
                dma((3, cblocks, 2)),
                dma((2,)),
                dma((2,)),
                dma((2, 2)),
                dma((2, 2)),
                dma((2, 2)),
                dma((2, 2)),
            ],
            compiler_params=pltpu.CompilerParams(
                collective_id=0, has_side_effects=True, vmem_limit_bytes=48 * 1024 * 1024),
            name="steps",
        )(*(pltpu.with_memory_space_constraint(x, pltpu.HBM) for x in (weights, gains, u_init, forcing, loss_weight)))

    return jax.shard_map(local_run, mesh=mesh, in_specs=(field_spec, field_spec, field_spec, P(), P()),
                         out_specs=(field_spec, field_spec, field_spec), check_vma=False)
```

```python
import functools

import jax
import jax.numpy as jnp
from jax import lax
from jax.experimental import pallas as pl
from jax.experimental.pallas import tpu as pltpu
from jax.sharding import PartitionSpec as P


DT = 0.01
LANES = 128
PHASE = 8
BANKED = 4
UNROLL = 8
MESH = pl.DeviceIdType.MESH


def stencil_blocks(load, wts, centre, nb):
    part = {}
    for b in range(nb):
        left, mid, right = load(b, -1), load(b, 0), load(b, 1)
        part[b, -1] = (wts[0][0] * left + wts[0][1] * mid) + wts[0][2] * right
        part[b, 0] = (wts[1][0] * left + centre(b, mid) * mid) + wts[1][2] * right
        part[b, 1] = (wts[2][0] * left + wts[2][1] * mid) + wts[2][2] * right
    part[-1, -1] = pltpu.roll(part[nb - 1, -1], 1, 1)
    part[nb, 1] = pltpu.roll(part[0, 1], LANES - 1, 1)
    return [(part[b - 1, -1] + part[b, 0]) + part[b + 1, 1] for b in range(nb)]


def kernel(row_size, col_size, core_size, tiles, wts_hbm, gains_hbm, u_hbm, f_hbm, w_hbm, uo_ref, lo_ref, ao_ref,
           wts_ref, gains_ref, nat, ubase, lbase, inner, coef, forces, par_sem, loc_sem, row_send, row_recv, f_send, f_recv,
           u_send, u_recv, l_send, l_recv):
    rows, width, steps = tiles
    force = acc = forces.at[0]
    nb = force.shape[0]
    halo = (nb * LANES - rows) // 2
    half = halo // 2
    fdep, adep = 2 * PHASE, PHASE
    org = fdep
    phases = steps // PHASE
    groups = width // 8
    scale = DT ** 0.5

    row_id, col_id, core_id = lax.axis_index("row"), lax.axis_index("col"), lax.axis_index("core")
    up, down = lax.rem(row_id + row_size - 1, row_size), lax.rem(row_id + 1, row_size)
    flat = col_id * core_size + core_id
    total = col_size * core_size
    lflat, rflat = lax.rem(flat + total - 1, total), lax.rem(flat + 1, total)
    above, below = {"row": up}, {"row": down}
    left = {"col": lax.div(lflat, core_size), "core": lax.rem(lflat, core_size)}
    right = {"col": lax.div(rflat, core_size), "core": lax.rem(rflat, core_size)}

    srcs = (u_hbm, f_hbm, w_hbm)
    cblocks = width // LANES
    local = [[pltpu.make_async_copy(srcs[k].at[:, pl.ds(cb * LANES, LANES)], nat.at[k, cb, pl.ds(halo, rows), :],
                                    loc_sem.at[k, cb]) for cb in range(cblocks)] for k in range(3)]
    for k in range(3):
        for copy in local[k]:
            copy.start()
    params = [pltpu.make_async_copy(wts_hbm, wts_ref, par_sem.at[0]),
              pltpu.make_async_copy(gains_hbm, gains_ref, par_sem.at[1])]
    for copy in params:
        copy.start()

    barrier = pltpu.get_barrier_semaphore()
    for dev in (above, below, left, right):
        pl.semaphore_signal(barrier, inc=1, device_id=dev, device_id_type=MESH)
    pl.semaphore_wait(barrier, 4)

    def row_copies(k):
        dep = halo if k < 2 else half
        out = []
        for cb in range(cblocks):
            out.append(pltpu.make_async_remote_copy(
                nat.at[k, cb, pl.ds(halo, dep), :], nat.at[k, cb, pl.ds(halo + rows, dep), :],
                row_send.at[k, cb, 0], row_recv.at[k, cb, 0], device_id=above, device_id_type=MESH))
            out.append(pltpu.make_async_remote_copy(
                nat.at[k, cb, pl.ds(halo + rows - dep, dep), :], nat.at[k, cb, pl.ds(halo - dep, dep), :],
                row_send.at[k, cb, 1], row_recv.at[k, cb, 1], device_id=below, device_id_type=MESH))
        return out

    def col_copies(ref, dep, send, recv):
        return [
            pltpu.make_async_remote_copy(ref.at[:, pl.ds(org, dep), :], ref.at[:, pl.ds(org + width, dep), :],
                                         send.at[0], recv.at[0], device_id=left, device_id_type=MESH),
            pltpu.make_async_remote_copy(ref.at[:, pl.ds(org + width - dep, dep), :], ref.at[:, pl.ds(org - dep, dep), :],
                                         send.at[1], recv.at[1], device_id=right, device_id_type=MESH),
        ]

    rcopies = [row_copies(k) for k in range(3)]
    for k in range(3):
        for copy in local[k]:
            copy.wait()
        for copy in rcopies[k]:
            copy.start()
    for copy in params:
        copy.wait()

    def arrive(k, dst, factor):
        for copy in rcopies[k]:
            copy.wait()
        for cb in range(cblocks):
            for b in range(nb):
                val = jnp.transpose(nat[k, cb, pl.ds(b, LANES, stride=nb), :])
                if factor is not None:
                    val = val * factor
                dst[b, pl.ds(org + cb * LANES, LANES), :] = val

    def depart(src, k, out, factor):
        for cb in range(cblocks):
            for b in range(nb):
                val = jnp.transpose(src[b, pl.ds(org + cb * LANES, LANES), :])
                if factor is not None:
                    val = val * factor
                nat[k, cb, pl.ds(b, LANES, stride=nb), :] = val
            out[:, pl.ds(cb * LANES, LANES)] = nat[k, cb, pl.ds(halo, rows), :]

    arrive(0, ubase.at[0], scale)
    for copy in col_copies(ubase.at[0], fdep, u_send.at[0], u_recv.at[0]):
        copy.start()
    arrive(1, force, scale)
    fcopies = col_copies(force, fdep, f_send, f_recv)
    for copy in fcopies:
        copy.start()

    wts = [[wts_ref[i, j] for j in range(3)] for i in range(3)]
    flip = [[wts_ref[2 - i, 2 - j] for j in range(3)] for i in range(3)]
    mid_wt = wts_ref[1, 1] + DT

    def sweep(body, base, count):
        for off in range(0, count, 8 * UNROLL):
            body(base + off, min(8 * UNROLL, count - off))

    def cover(step_body, dep):
        def middle():
            for j in range(1, PHASE + 1):
                sweep(functools.partial(step_body, j), org + j, width - 2 * j)

        def sides():
            for j in range(1, PHASE):
                sweep(functools.partial(step_body, j), org + j - dep, dep)
                sweep(functools.partial(step_body, j), org + width - j, dep)
            sweep(functools.partial(step_body, PHASE), org, PHASE)
            sweep(functools.partial(step_body, PHASE), org + width - PHASE, PHASE)
        return middle, sides

    def level(base, par, j):
        if j == 0:
            return base.at[par * BANKED]
        return base.at[(1 - par) * BANKED] if j == PHASE else inner.at[j - 1]

    def reaction(val, t, b, at):
        sq = val * val
        weight = mid_wt - sq
        coef[t, b, at, :] = (weight - sq) - sq
        return weight

    def fwd_phase(phase, _):
        par = lax.rem(phase, 2)

        def step_body(j, base, cols):
            src, dst, t = level(ubase, par, j - 1), level(ubase, par, j), phase * PHASE + (j - 1)
            gain = gains_ref[t]
            at = pl.ds(base, cols)

            def centre(b, mid):
                return reaction(mid, t, b, at)
            sums = stencil_blocks(lambda b, d: src[b, pl.ds(base + d, cols), :], wts, centre, nb)
            for b in range(nb):
                dst[b, at, :] = sums[b] + gain * force[b, at, :]

        middle, sides = cover(step_body, fdep)
        middle()
        for copy in col_copies(ubase.at[par * BANKED], fdep, u_send.at[par], u_recv.at[par]):
            copy.wait()

        @pl.when(phase == 0)
        def _():
            for copy in fcopies:
                copy.wait()
        sides()
        last = phase * PHASE + (PHASE - 1)
        for at in (pl.ds(org - PHASE, PHASE), pl.ds(org + width, PHASE)):
            for b in range(nb):
                reaction(inner[PHASE - 2, b, at, :], last, b, at)

        @pl.when(phase < phases - 1)
        def _():
            for copy in col_copies(ubase.at[(1 - par) * BANKED], fdep, u_send.at[1 - par], u_recv.at[1 - par]):
                copy.start()
        return 0

    lax.fori_loop(0, phases, fwd_phase, 0)

    arrive(2, lbase.at[0], None)
    for copy in col_copies(lbase.at[0], adep, l_send.at[0], l_recv.at[0]):
        copy.start()
    depart(ubase.at[phases % 2 * BANKED], 0, uo_ref, 1.0 / scale)
    acc[...] = jnp.zeros(acc.shape, jnp.float32)

    def adj_phase(phase, _):
        par = lax.rem(phase, 2)

        def step_body(j, base, cols):
            src, dst, t = level(lbase, par, j - 1), level(lbase, par, j), steps - (phase * PHASE + j)
            gain = gains_ref[t]
            at = pl.ds(base, cols)

            def centre(b, mid):
                acc[b, at, :] += gain * mid
                return coef[t, b, at, :]
            sums = stencil_blocks(lambda b, d: src[b, pl.ds(base + d, cols), :], flip, centre, nb)
            for b in range(nb):
                dst[b, at, :] = sums[b]

        middle, sides = cover(step_body, adep)
        middle()
        for copy in col_copies(lbase.at[par * BANKED], adep, l_send.at[par], l_recv.at[par]):
            copy.wait()
        sides()

        @pl.when(phase < phases - 1)
        def _():
            for copy in col_copies(lbase.at[(1 - par) * BANKED], adep, l_send.at[1 - par], l_recv.at[1 - par]):
                copy.start()
        return 0

    lax.fori_loop(0, phases, adj_phase, 0)

    lo_ref[...] = lbase[phases % 2 * BANKED, :, pl.ds(org, width), :]
    ao_ref[...] = acc[:, pl.ds(org, width), :]


def unlane(tiles, u_ref, l_ref, a_ref, uo_hbm, go_hbm, gf_hbm, nat, sem):
    rows, width = tiles
    nb = l_ref.shape[0]
    halo = (nb * LANES - rows) // 2
    copies = [pltpu.make_async_copy(u_ref, uo_hbm, sem.at[0, 0])]
    copies[0].start()
    for k, (src, out) in enumerate(((l_ref, go_hbm), (a_ref, gf_hbm))):
        for cb in range(width // LANES):
            for b in range(nb):
                nat[k, cb, pl.ds(b, LANES, stride=nb), :] = jnp.transpose(src[b, pl.ds(cb * LANES, LANES), :])
            copies.append(pltpu.make_async_copy(nat.at[k, cb, pl.ds(halo, rows), :],
                                                out.at[:, pl.ds(cb * LANES, LANES)], sem.at[k + 1, cb]))
            copies[-1].start()
    for copy in copies:
        copy.wait()


def solution(mesh):
    row_size, col_size, core_size = mesh.shape["row"], mesh.shape["col"], mesh.shape["core"]
    field_spec = P(("mem", "row"), ("col", "core"))

    def local_run(u_init, forcing, loss_weight, weights, gains):
        rows, width = u_init.shape
        steps = gains.shape[0]
        nb = -(-(rows + 4 * steps) // LANES)
        cols = width + 4 * PHASE + 8
        cblocks = width // LANES
        f32 = jnp.float32
        field = (nb, cols, LANES)
        dma = pltpu.SemaphoreType.DMA
        hbm, vmem = pl.BlockSpec(memory_space=pl.ANY), pl.BlockSpec(memory_space=pltpu.VMEM)
        lanes_out = pl.pallas_call(
            functools.partial(kernel, row_size, col_size, core_size, (rows, width, steps)),
            out_shape=[jax.ShapeDtypeStruct(dims, f32) for dims in ((rows, width), (nb, width, LANES), (nb, width, LANES))],
            in_specs=[hbm] * 5,
            out_specs=[vmem, vmem, vmem],
            scratch_shapes=[
                pltpu.SMEM(weights.shape, f32),
                pltpu.SMEM(gains.shape, f32),
                pltpu.VMEM((3, cblocks, nb * LANES, LANES), f32),
                pltpu.VMEM((2 * BANKED,) + field, f32),
                pltpu.VMEM((2 * BANKED,) + field, f32),
                pltpu.VMEM((PHASE,) + field, f32),
                pltpu.VMEM((steps,) + field, f32),
                pltpu.VMEM((BANKED,) + field, f32),
                dma((2,)),
                dma((3, cblocks)),
                dma((3, cblocks, 2)),
                dma((3, cblocks, 2)),
                dma((2,)),
                dma((2,)),
                dma((2, 2)),
                dma((2, 2)),
                dma((2, 2)),
                dma((2, 2)),
            ],
            compiler_params=pltpu.CompilerParams(
                collective_id=0, has_side_effects=True, vmem_limit_bytes=52 * 1024 * 1024),
            name="steps",
        )(*(pltpu.with_memory_space_constraint(x, pltpu.HBM) for x in (weights, gains, u_init, forcing, loss_weight)))
        return pl.pallas_call(
            functools.partial(unlane, (rows, width)),
            out_shape=[jax.ShapeDtypeStruct((rows, width), f32)] * 3,
            in_specs=[vmem] * 3,
            out_specs=[hbm] * 3,
            scratch_shapes=[pltpu.VMEM((2, cblocks, nb * LANES, LANES), f32), dma((3, 2))],
            compiler_params=pltpu.CompilerParams(vmem_limit_bytes=16 * 1024 * 1024),
            name="unlane",
        )(*(pltpu.with_memory_space_constraint(x, pltpu.VMEM) for x in lanes_out))

    return jax.shard_map(local_run, mesh=mesh, in_specs=(field_spec, field_spec, field_spec, P(), P()),
                         out_specs=(field_spec, field_spec, field_spec), check_vma=False)
```

```python
import functools

import jax
import jax.numpy as jnp
from jax import lax
from jax.experimental import pallas as pl
from jax.experimental.pallas import tpu as pltpu
from jax.sharding import PartitionSpec as P


DT = 0.01
LANES = 128
PHASE = 8
BANKED = 4
UNROLL = 8
MESH = pl.DeviceIdType.MESH


def stencil_blocks(load, wts, centre, nb):
    part = {}
    for b in range(nb):
        left, mid, right = load(b, -1), load(b, 0), load(b, 1)
        part[b, -1] = (wts[0][0] * left + wts[0][1] * mid) + wts[0][2] * right
        part[b, 0] = (wts[1][0] * left + centre(b, mid) * mid) + wts[1][2] * right
        part[b, 1] = (wts[2][0] * left + wts[2][1] * mid) + wts[2][2] * right
    part[-1, -1] = pltpu.roll(part[nb - 1, -1], 1, 1)
    part[nb, 1] = pltpu.roll(part[0, 1], LANES - 1, 1)
    return [(part[b - 1, -1] + part[b, 0]) + part[b + 1, 1] for b in range(nb)]


def kernel(row_size, col_size, core_size, tiles, wts_hbm, gains_hbm, u_hbm, f_hbm, w_hbm, uo_ref, lo_ref, ao_ref,
           wts_ref, gains_ref, nat, ubase, lbase, inner, coef, forces, par_sem, loc_sem, row_send, row_recv, f_send, f_recv,
           u_send, u_recv, l_send, l_recv):
    rows, width, steps = tiles
    force = acc = forces.at[0]
    nb = force.shape[0]
    halo = (nb * LANES - rows) // 2
    half = halo // 2
    fdep, adep = 2 * PHASE, PHASE
    org = fdep
    phases = steps // PHASE
    groups = width // 8
    scale = DT ** 0.5

    row_id, col_id, core_id = lax.axis_index("row"), lax.axis_index("col"), lax.axis_index("core")
    up, down = lax.rem(row_id + row_size - 1, row_size), lax.rem(row_id + 1, row_size)
    flat = col_id * core_size + core_id
    total = col_size * core_size
    lflat, rflat = lax.rem(flat + total - 1, total), lax.rem(flat + 1, total)
    above, below = {"row": up}, {"row": down}
    left = {"col": lax.div(lflat, core_size), "core": lax.rem(lflat, core_size)}
    right = {"col": lax.div(rflat, core_size), "core": lax.rem(rflat, core_size)}

    srcs = (u_hbm, f_hbm, w_hbm)
    cblocks = width // LANES
    local = [[pltpu.make_async_copy(srcs[k].at[:, pl.ds(cb * LANES, LANES)], nat.at[k, cb, pl.ds(halo, rows), :],
                                    loc_sem.at[k, cb]) for cb in range(cblocks)] for k in range(3)]
    for k in range(3):
        for copy in local[k]:
            copy.start()
    params = [pltpu.make_async_copy(wts_hbm, wts_ref, par_sem.at[0]),
              pltpu.make_async_copy(gains_hbm, gains_ref, par_sem.at[1])]
    for copy in params:
        copy.start()

    barrier = pltpu.get_barrier_semaphore()
    for dev in (above, below, left, right):
        pl.semaphore_signal(barrier, inc=1, device_id=dev, device_id_type=MESH)
    pl.semaphore_wait(barrier, 4)

    def row_copies(k):
        dep = halo if k < 2 else half
        strip = lambda first: nat.at[k, :, pl.ds(first, dep), :]
        return [
            pltpu.make_async_remote_copy(strip(halo), strip(halo + rows), row_send.at[k, 0], row_recv.at[k, 0],
                                         device_id=above, device_id_type=MESH),
            pltpu.make_async_remote_copy(strip(halo + rows - dep), strip(halo - dep), row_send.at[k, 1],
                                         row_recv.at[k, 1], device_id=below, device_id_type=MESH),
        ]

    def col_copies(ref, dep, send, recv):
        return [
            pltpu.make_async_remote_copy(ref.at[:, pl.ds(org, dep), :], ref.at[:, pl.ds(org + width, dep), :],
                                         send.at[0], recv.at[0], device_id=left, device_id_type=MESH),
            pltpu.make_async_remote_copy(ref.at[:, pl.ds(org + width - dep, dep), :], ref.at[:, pl.ds(org - dep, dep), :],
                                         send.at[1], recv.at[1], device_id=right, device_id_type=MESH),
        ]

    rcopies = [row_copies(k) for k in range(3)]
    for k in range(3):
        for copy in local[k]:
            copy.wait()
        for copy in rcopies[k]:
            copy.start()
    for copy in params:
        copy.wait()

    def arrive(k, dst, factor):
        for copy in rcopies[k]:
            copy.wait()
        for cb in range(cblocks):
            for b in range(nb):
                val = jnp.transpose(nat[k, cb, pl.ds(b, LANES, stride=nb), :])
                if factor is not None:
                    val = val * factor
                dst[b, pl.ds(org + cb * LANES, LANES), :] = val

    def depart(src, k, out, factor):
        for cb in range(cblocks):
            for b in range(nb):
                val = jnp.transpose(src[b, pl.ds(org + cb * LANES, LANES), :])
                if factor is not None:
                    val = val * factor
                nat[k, cb, pl.ds(b, LANES, stride=nb), :] = val
            out[:, pl.ds(cb * LANES, LANES)] = nat[k, cb, pl.ds(halo, rows), :]

    arrive(0, ubase.at[0], scale)
    for copy in col_copies(ubase.at[0], fdep, u_send.at[0], u_recv.at[0]):
        copy.start()
    wts = [[wts_ref[i, j] for j in range(3)] for i in range(3)]
    flip = [[wts_ref[2 - i, 2 - j] for j in range(3)] for i in range(3)]
    mid_wt = wts_ref[1, 1] + DT

    def sweep(body, base, count):
        for off in range(0, count, 8 * UNROLL):
            body(base + off, min(8 * UNROLL, count - off))

    def cover(step_body, dep):
        def first():
            sweep(functools.partial(step_body, 1), org + 1, width - 2)

        def middle():
            for j in range(2, PHASE + 1):
                sweep(functools.partial(step_body, j), org + j, width - 2 * j)

        def sides():
            for j in range(1, PHASE):
                sweep(functools.partial(step_body, j), org + j - dep, dep)
                sweep(functools.partial(step_body, j), org + width - j, dep)
            sweep(functools.partial(step_body, PHASE), org, PHASE)
            sweep(functools.partial(step_body, PHASE), org + width - PHASE, PHASE)
        return first, middle, sides

    def level(base, par, j):
        if j == 0:
            return base.at[par * BANKED]
        return base.at[(1 - par) * BANKED] if j == PHASE else inner.at[j - 1]

    def reaction(val, t, b, at):
        sq = val * val
        weight = mid_wt - sq
        coef[t, b, at, :] = (weight - sq) - sq
        return weight

    def fwd_body(phase, forced, j, base, cols):
        par = lax.rem(phase, 2)
        src, dst, t = level(ubase, par, j - 1), level(ubase, par, j), phase * PHASE + (j - 1)
        at = pl.ds(base, cols)
        sums = stencil_blocks(lambda b, d: src[b, pl.ds(base + d, cols), :], wts,
                              lambda b, mid: reaction(mid, t, b, at), nb)
        for b in range(nb):
            dst[b, at, :] = sums[b] + gains_ref[t] * force[b, at, :] if forced else sums[b]

    sweep(functools.partial(fwd_body, 0, False, 1), org + 1, width - 2)
    arrive(1, force, scale)
    fcopies = col_copies(force, fdep, f_send, f_recv)
    for copy in fcopies:
        copy.start()

    for b in range(nb):
        at = pl.ds(org + 1, width - 2)
        inner[0, b, at, :] = inner[0, b, at, :] + gains_ref[0] * force[b, at, :]

    def fwd_phase(phase, _):
        par = lax.rem(phase, 2)
        step_body = functools.partial(fwd_body, phase, True)
        first, middle, sides = cover(step_body, fdep)
        pl.when(phase > 0)(first)
        middle()
        for copy in col_copies(ubase.at[par * BANKED], fdep, u_send.at[par], u_recv.at[par]):
            copy.wait()

        @pl.when(phase == 0)
        def _():
            for copy in fcopies:
                copy.wait()
        sides()
        last = phase * PHASE + (PHASE - 1)
        for at in (pl.ds(org - PHASE, PHASE), pl.ds(org + width, PHASE)):
            for b in range(nb):
                reaction(inner[PHASE - 2, b, at, :], last, b, at)

        @pl.when(phase < phases - 1)
        def _():
            for copy in col_copies(ubase.at[(1 - par) * BANKED], fdep, u_send.at[1 - par], u_recv.at[1 - par]):
                copy.start()
        return 0

    lax.fori_loop(0, phases, fwd_phase, 0)

    arrive(2, lbase.at[0], None)
    for copy in col_copies(lbase.at[0], adep, l_send.at[0], l_recv.at[0]):
        copy.start()
    depart(ubase.at[phases % 2 * BANKED], 0, uo_ref, 1.0 / scale)
    acc[...] = jnp.zeros(acc.shape, jnp.float32)

    def adj_phase(phase, _):
        par = lax.rem(phase, 2)

        def step_body(j, base, cols):
            src, dst, t = level(lbase, par, j - 1), level(lbase, par, j), steps - (phase * PHASE + j)
            gain = gains_ref[t]
            at = pl.ds(base, cols)

            def centre(b, mid):
                acc[b, at, :] += gain * mid
                return coef[t, b, at, :]
            sums = stencil_blocks(lambda b, d: src[b, pl.ds(base + d, cols), :], flip, centre, nb)
            for b in range(nb):
                dst[b, at, :] = sums[b]

        first, middle, sides = cover(step_body, adep)
        first()
        middle()
        for copy in col_copies(lbase.at[par * BANKED], adep, l_send.at[par], l_recv.at[par]):
            copy.wait()
        sides()

        @pl.when(phase < phases - 1)
        def _():
            for copy in col_copies(lbase.at[(1 - par) * BANKED], adep, l_send.at[1 - par], l_recv.at[1 - par]):
                copy.start()
        return 0

    lax.fori_loop(0, phases, adj_phase, 0)

    lo_ref[...] = lbase[phases % 2 * BANKED, :, pl.ds(org, width), :]
    ao_ref[...] = acc[:, pl.ds(org, width), :]


def unlane(tiles, u_ref, l_ref, a_ref, uo_hbm, go_hbm, gf_hbm, nat, sem):
    rows, width = tiles
    nb = l_ref.shape[0]
    halo = (nb * LANES - rows) // 2
    copies = [pltpu.make_async_copy(u_ref, uo_hbm, sem.at[0, 0])]
    copies[0].start()
    for k, (src, out) in enumerate(((l_ref, go_hbm), (a_ref, gf_hbm))):
        for cb in range(width // LANES):
            for b in range(nb):
                nat[k, cb, pl.ds(b, LANES, stride=nb), :] = jnp.transpose(src[b, pl.ds(cb * LANES, LANES), :])
            copies.append(pltpu.make_async_copy(nat.at[k, cb, pl.ds(halo, rows), :],
                                                out.at[:, pl.ds(cb * LANES, LANES)], sem.at[k + 1, cb]))
            copies[-1].start()
    for copy in copies:
        copy.wait()


def solution(mesh):
    row_size, col_size, core_size = mesh.shape["row"], mesh.shape["col"], mesh.shape["core"]
    field_spec = P(("mem", "row"), ("col", "core"))

    def local_run(u_init, forcing, loss_weight, weights, gains):
        rows, width = u_init.shape
        steps = gains.shape[0]
        nb = -(-(rows + 4 * steps) // LANES)
        cols = width + 4 * PHASE + 8
        cblocks = width // LANES
        f32 = jnp.float32
        field = (nb, cols, LANES)
        dma = pltpu.SemaphoreType.DMA
        hbm, vmem = pl.BlockSpec(memory_space=pl.ANY), pl.BlockSpec(memory_space=pltpu.VMEM)
        lanes_out = pl.pallas_call(
            functools.partial(kernel, row_size, col_size, core_size, (rows, width, steps)),
            out_shape=[jax.ShapeDtypeStruct(dims, f32) for dims in ((rows, width), (nb, width, LANES), (nb, width, LANES))],
            in_specs=[hbm] * 5,
            out_specs=[vmem, vmem, vmem],
            scratch_shapes=[
                pltpu.SMEM(weights.shape, f32),
                pltpu.SMEM(gains.shape, f32),
                pltpu.VMEM((3, cblocks, nb * LANES, LANES), f32),
                pltpu.VMEM((2 * BANKED,) + field, f32),
                pltpu.VMEM((2 * BANKED,) + field, f32),
                pltpu.VMEM((PHASE,) + field, f32),
                pltpu.VMEM((steps,) + field, f32),
                pltpu.VMEM((BANKED,) + field, f32),
                dma((2,)),
                dma((3, cblocks)),
                dma((3, 2)),
                dma((3, 2)),
                dma((2,)),
                dma((2,)),
                dma((2, 2)),
                dma((2, 2)),
                dma((2, 2)),
                dma((2, 2)),
            ],
            compiler_params=pltpu.CompilerParams(
                collective_id=0, has_side_effects=True, vmem_limit_bytes=52 * 1024 * 1024),
            name="steps",
        )(*(pltpu.with_memory_space_constraint(x, pltpu.HBM) for x in (weights, gains, u_init, forcing, loss_weight)))
        return pl.pallas_call(
            functools.partial(unlane, (rows, width)),
            out_shape=[jax.ShapeDtypeStruct((rows, width), f32)] * 3,
            in_specs=[vmem] * 3,
            out_specs=[hbm] * 3,
            scratch_shapes=[pltpu.VMEM((2, cblocks, nb * LANES, LANES), f32), dma((3, 2))],
            compiler_params=pltpu.CompilerParams(vmem_limit_bytes=16 * 1024 * 1024),
            name="unlane",
        )(*(pltpu.with_memory_space_constraint(x, pltpu.VMEM) for x in lanes_out))

    return jax.shard_map(local_run, mesh=mesh, in_specs=(field_spec, field_spec, field_spec, P(), P()),
                         out_specs=(field_spec, field_spec, field_spec), check_vma=False)
```

```python
import functools

import jax
import jax.numpy as jnp
from jax import lax
from jax.experimental import pallas as pl
from jax.experimental.pallas import tpu as pltpu
from jax.sharding import PartitionSpec as P


DT = 0.01
LANES = 128
PHASE = 8
BANKED = 4
UNROLL = 8
MESH = pl.DeviceIdType.MESH


def stencil_blocks(load, wts, centre, nb):
    part = {}
    for b in range(nb):
        left, mid, right = load(b, -1), load(b, 0), load(b, 1)
        part[b, -1] = (wts[0][0] * left + wts[0][1] * mid) + wts[0][2] * right
        part[b, 0] = (wts[1][0] * left + centre(b, mid) * mid) + wts[1][2] * right
        part[b, 1] = (wts[2][0] * left + wts[2][1] * mid) + wts[2][2] * right
    part[-1, -1] = pltpu.roll(part[nb - 1, -1], 1, 1)
    part[nb, 1] = pltpu.roll(part[0, 1], LANES - 1, 1)
    return [(part[b - 1, -1] + part[b, 0]) + part[b + 1, 1] for b in range(nb)]


def kernel(row_size, col_size, core_size, tiles, wts_hbm, gains_hbm, u_hbm, f_hbm, w_hbm, uo_ref, lo_ref, ao_ref,
           wts_ref, gains_ref, nat, ubase, lbase, inner, coef, forces, par_sem, loc_sem, row_send, row_recv, f_send, f_recv,
           u_send, u_recv, l_send, l_recv):
    rows, width, steps = tiles
    force, acc = forces.at[0], ao_ref
    nb = force.shape[0]
    halo = (nb * LANES - rows) // 2
    half = halo // 2
    fdep, adep = 2 * PHASE, PHASE
    org = fdep
    phases = steps // PHASE
    groups = width // 8
    scale = DT ** 0.5

    row_id, col_id, core_id = lax.axis_index("row"), lax.axis_index("col"), lax.axis_index("core")
    up, down = lax.rem(row_id + row_size - 1, row_size), lax.rem(row_id + 1, row_size)
    flat = col_id * core_size + core_id
    total = col_size * core_size
    lflat, rflat = lax.rem(flat + total - 1, total), lax.rem(flat + 1, total)
    above, below = {"row": up}, {"row": down}
    left = {"col": lax.div(lflat, core_size), "core": lax.rem(lflat, core_size)}
    right = {"col": lax.div(rflat, core_size), "core": lax.rem(rflat, core_size)}

    barrier = pltpu.get_barrier_semaphore()
    for dev in (above, below, left, right):
        pl.semaphore_signal(barrier, inc=1, device_id=dev, device_id_type=MESH)

    srcs = (u_hbm, f_hbm, w_hbm)
    cblocks = width // LANES

    def fetch(k):
        dep = halo if k < 2 else half

        def part(n, first, count):
            return [pltpu.make_async_copy(
                srcs[k].at[pl.ds(first, count), pl.ds(cb * LANES, LANES)],
                nat.at[k, cb, pl.ds(halo + first, count), :], loc_sem.at[k, cb, n]) for cb in range(cblocks)]
        return part(0, 0, dep) + part(1, rows - dep, dep), part(2, dep, rows - 2 * dep)

    local = [fetch(k) for k in range(3)]
    for copy in local[0][0] + local[0][1]:
        copy.start()
    params = [pltpu.make_async_copy(wts_hbm, wts_ref, par_sem.at[0]),
              pltpu.make_async_copy(gains_hbm, gains_ref, par_sem.at[1])]
    for copy in params:
        copy.start()
    for k in (1, 2):
        for copy in local[k][0] + local[k][1]:
            copy.start()
    pl.semaphore_wait(barrier, 4)

    def row_copies(k):
        dep = halo if k < 2 else half
        strip = lambda first: nat.at[k, :, pl.ds(first, dep), :]
        return [
            pltpu.make_async_remote_copy(strip(halo), strip(halo + rows), row_send.at[k, 0], row_recv.at[k, 0],
                                         device_id=above, device_id_type=MESH),
            pltpu.make_async_remote_copy(strip(halo + rows - dep), strip(halo - dep), row_send.at[k, 1],
                                         row_recv.at[k, 1], device_id=below, device_id_type=MESH),
        ]

    def col_copies(ref, dep, send, recv):
        return [
            pltpu.make_async_remote_copy(ref.at[:, pl.ds(org, dep), :], ref.at[:, pl.ds(org + width, dep), :],
                                         send.at[0], recv.at[0], device_id=left, device_id_type=MESH),
            pltpu.make_async_remote_copy(ref.at[:, pl.ds(org + width - dep, dep), :], ref.at[:, pl.ds(org - dep, dep), :],
                                         send.at[1], recv.at[1], device_id=right, device_id_type=MESH),
        ]

    rcopies = [row_copies(k) for k in range(3)]
    for k in range(3):
        for copy in local[k][0]:
            copy.wait()
        for copy in rcopies[k]:
            copy.start()
    for copy in params:
        copy.wait()

    def arrive(k, dst, factor):
        for copy in local[k][1] + rcopies[k]:
            copy.wait()
        for cb in range(cblocks):
            for b in range(nb):
                val = jnp.transpose(nat[k, cb, pl.ds(b, LANES, stride=nb), :])
                if factor is not None:
                    val = val * factor
                dst[b, pl.ds(org + cb * LANES, LANES), :] = val

    def depart(src, k, out, factor):
        for cb in range(cblocks):
            for b in range(nb):
                val = jnp.transpose(src[b, pl.ds(org + cb * LANES, LANES), :])
                if factor is not None:
                    val = val * factor
                nat[k, cb, pl.ds(b, LANES, stride=nb), :] = val
            out[:, pl.ds(cb * LANES, LANES)] = nat[k, cb, pl.ds(halo, rows), :]

    arrive(0, ubase.at[0], scale)
    for copy in col_copies(ubase.at[0], fdep, u_send.at[0], u_recv.at[0]):
        copy.start()
    wts = [[wts_ref[i, j] for j in range(3)] for i in range(3)]
    flip = [[wts_ref[2 - i, 2 - j] for j in range(3)] for i in range(3)]
    mid_wt = wts_ref[1, 1] + DT

    def sweep(body, base, count):
        for off in range(0, count, 8 * UNROLL):
            body(base + off, min(8 * UNROLL, count - off))

    def cover(step_body, dep):
        def first():
            sweep(functools.partial(step_body, 1), org + 1, width - 2)

        def middle():
            for j in range(2, PHASE + 1):
                sweep(functools.partial(step_body, j), org + j, width - 2 * j)

        def sides():
            for j in range(1, PHASE):
                sweep(functools.partial(step_body, j), org + j - dep, dep)
                sweep(functools.partial(step_body, j), org + width - j, dep)
            sweep(functools.partial(step_body, PHASE), org, PHASE)
            sweep(functools.partial(step_body, PHASE), org + width - PHASE, PHASE)
        return first, middle, sides

    def level(base, par, j):
        if j == 0:
            return base.at[par * BANKED]
        return base.at[(1 - par) * BANKED] if j == PHASE else inner.at[j - 1]

    def reaction(val, t, b, at):
        sq = val * val
        weight = mid_wt - sq
        coef[t, b, at, :] = (weight - sq) - sq
        return weight

    def fwd_body(phase, forced, j, base, cols):
        par = lax.rem(phase, 2)
        src, dst, t = level(ubase, par, j - 1), level(ubase, par, j), phase * PHASE + (j - 1)
        at = pl.ds(base, cols)
        sums = stencil_blocks(lambda b, d: src[b, pl.ds(base + d, cols), :], wts,
                              lambda b, mid: reaction(mid, t, b, at), nb)
        for b in range(nb):
            dst[b, at, :] = sums[b] + gains_ref[t] * force[b, at, :] if forced else sums[b]

    sweep(functools.partial(fwd_body, 0, False, 1), org + 1, width - 2)
    arrive(1, force, scale)
    fcopies = col_copies(force, fdep, f_send, f_recv)
    for copy in fcopies:
        copy.start()

    for b in range(nb):
        at = pl.ds(org + 1, width - 2)
        inner[0, b, at, :] = inner[0, b, at, :] + gains_ref[0] * force[b, at, :]

    def fwd_phase(phase, _):
        par = lax.rem(phase, 2)
        step_body = functools.partial(fwd_body, phase, True)
        first, middle, sides = cover(step_body, fdep)
        pl.when(phase > 0)(first)
        middle()
        for copy in col_copies(ubase.at[par * BANKED], fdep, u_send.at[par], u_recv.at[par]):
            copy.wait()

        @pl.when(phase == 0)
        def _():
            for copy in fcopies:
                copy.wait()
        sides()
        last = phase * PHASE + (PHASE - 1)
        for at in (pl.ds(org - PHASE, PHASE), pl.ds(org + width, PHASE)):
            for b in range(nb):
                reaction(inner[PHASE - 2, b, at, :], last, b, at)

        @pl.when(phase < phases - 1)
        def _():
            for copy in col_copies(ubase.at[(1 - par) * BANKED], fdep, u_send.at[1 - par], u_recv.at[1 - par]):
                copy.start()
        return 0

    lax.fori_loop(0, phases, fwd_phase, 0)

    arrive(2, lbase.at[0], None)
    for copy in col_copies(lbase.at[0], adep, l_send.at[0], l_recv.at[0]):
        copy.start()
    depart(ubase.at[phases % 2 * BANKED], 0, uo_ref, 1.0 / scale)
    acc[...] = jnp.zeros(acc.shape, jnp.float32)

    def adj_phase(phase, _):
        par = lax.rem(phase, 2)

        def step_body(j, base, cols):
            src, dst, t = level(lbase, par, j - 1), level(lbase, par, j), steps - (phase * PHASE + j)
            gain = gains_ref[t]
            at = pl.ds(base, cols)

            def centre(b, mid):
                acc[b, at, :] += gain * mid
                return coef[t, b, at, :]
            sums = stencil_blocks(lambda b, d: src[b, pl.ds(base + d, cols), :], flip, centre, nb)
            for b in range(nb):
                dst[b, at, :] = sums[b]

        first, middle, sides = cover(step_body, adep)
        first()
        middle()
        for copy in col_copies(lbase.at[par * BANKED], adep, l_send.at[par], l_recv.at[par]):
            copy.wait()
        sides()

        @pl.when(phase < phases - 1)
        def _():
            for copy in col_copies(lbase.at[(1 - par) * BANKED], adep, l_send.at[1 - par], l_recv.at[1 - par]):
                copy.start()
        return 0

    lax.fori_loop(0, phases, adj_phase, 0)

    lo_ref[...] = lbase[phases % 2 * BANKED, :, pl.ds(org, width), :]


def unlane(tiles, org, u_ref, l_ref, a_ref, uo_hbm, go_hbm, gf_hbm, nat, sem):
    rows, width = tiles
    nb = l_ref.shape[0]
    halo = (nb * LANES - rows) // 2
    copies = [pltpu.make_async_copy(u_ref, uo_hbm, sem.at[0, 0])]
    copies[0].start()
    for k, (src, first, out) in enumerate(((l_ref, 0, go_hbm), (a_ref, org, gf_hbm))):
        for cb in range(width // LANES):
            for b in range(nb):
                nat[k, cb, pl.ds(b, LANES, stride=nb), :] = jnp.transpose(src[b, pl.ds(first + cb * LANES, LANES), :])
            copies.append(pltpu.make_async_copy(nat.at[k, cb, pl.ds(halo, rows), :],
                                                out.at[:, pl.ds(cb * LANES, LANES)], sem.at[k + 1, cb]))
            copies[-1].start()
    for copy in copies:
        copy.wait()


def solution(mesh):
    row_size, col_size, core_size = mesh.shape["row"], mesh.shape["col"], mesh.shape["core"]
    field_spec = P(("mem", "row"), ("col", "core"))

    def local_run(u_init, forcing, loss_weight, weights, gains):
        rows, width = u_init.shape
        steps = gains.shape[0]
        nb = -(-(rows + 4 * steps) // LANES)
        cols = width + 4 * PHASE + 8
        cblocks = width // LANES
        f32 = jnp.float32
        field = (nb, cols, LANES)
        dma = pltpu.SemaphoreType.DMA
        hbm, vmem = pl.BlockSpec(memory_space=pl.ANY), pl.BlockSpec(memory_space=pltpu.VMEM)
        lanes_out = pl.pallas_call(
            functools.partial(kernel, row_size, col_size, core_size, (rows, width, steps)),
            out_shape=[jax.ShapeDtypeStruct(dims, f32) for dims in ((rows, width), (nb, width, LANES), field)],
            in_specs=[hbm] * 5,
            out_specs=[vmem, vmem, vmem],
            scratch_shapes=[
                pltpu.SMEM(weights.shape, f32),
                pltpu.SMEM(gains.shape, f32),
                pltpu.VMEM((3, cblocks, nb * LANES, LANES), f32),
                pltpu.VMEM((2 * BANKED,) + field, f32),
                pltpu.VMEM((2 * BANKED,) + field, f32),
                pltpu.VMEM((PHASE,) + field, f32),
                pltpu.VMEM((steps,) + field, f32),
                pltpu.VMEM((BANKED,) + field, f32),
                dma((2,)),
                dma((3, cblocks, 3)),
                dma((3, 2)),
                dma((3, 2)),
                dma((2,)),
                dma((2,)),
                dma((2, 2)),
                dma((2, 2)),
                dma((2, 2)),
                dma((2, 2)),
            ],
            compiler_params=pltpu.CompilerParams(
                collective_id=0, has_side_effects=True, vmem_limit_bytes=52 * 1024 * 1024),
            name="steps",
        )(*(pltpu.with_memory_space_constraint(x, pltpu.HBM) for x in (weights, gains, u_init, forcing, loss_weight)))
        return pl.pallas_call(
            functools.partial(unlane, (rows, width), 2 * PHASE),
            out_shape=[jax.ShapeDtypeStruct((rows, width), f32)] * 3,
            in_specs=[vmem] * 3,
            out_specs=[hbm] * 3,
            scratch_shapes=[pltpu.VMEM((2, cblocks, nb * LANES, LANES), f32), dma((3, 2))],
            compiler_params=pltpu.CompilerParams(vmem_limit_bytes=16 * 1024 * 1024),
            name="unlane",
        )(*(pltpu.with_memory_space_constraint(x, pltpu.VMEM) for x in lanes_out))

    return jax.shard_map(local_run, mesh=mesh, in_specs=(field_spec, field_spec, field_spec, P(), P()),
                         out_specs=(field_spec, field_spec, field_spec), check_vma=False)
```

```python
import functools

import jax
import jax.numpy as jnp
from jax import lax
from jax.experimental import pallas as pl
from jax.experimental.pallas import tpu as pltpu
from jax.sharding import PartitionSpec as P


DT = 0.01
LANES = 128
PHASE = 8
BANKED = 4
UNROLL = 32
MESH = pl.DeviceIdType.MESH


def stencil_blocks(load, wts, centre, nb):
    part = {}
    for b in range(nb):
        left, mid, right = load(b, -1), load(b, 0), load(b, 1)
        part[b, -1] = (wts[0][0] * left + wts[0][1] * mid) + wts[0][2] * right
        part[b, 0] = (wts[1][0] * left + centre(b, mid) * mid) + wts[1][2] * right
        part[b, 1] = (wts[2][0] * left + wts[2][1] * mid) + wts[2][2] * right
    part[-1, -1] = pltpu.roll(part[nb - 1, -1], 1, 1)
    part[nb, 1] = pltpu.roll(part[0, 1], LANES - 1, 1)
    return [(part[b - 1, -1] + part[b, 0]) + part[b + 1, 1] for b in range(nb)]


def kernel(row_size, col_size, core_size, tiles, wts_hbm, gains_hbm, u_hbm, f_hbm, w_hbm, uo_ref, lo_ref, ao_ref,
           wts_ref, gains_ref, nat, ubase, lbase, inner, coef, forces, par_sem, loc_sem, row_send, row_recv, f_send, f_recv,
           u_send, u_recv, l_send, l_recv):
    rows, width, steps = tiles
    force, acc = forces.at[0], ao_ref
    nb = force.shape[0]
    halo = (nb * LANES - rows) // 2
    half = halo // 2
    fdep, adep = 2 * PHASE, PHASE
    org = fdep
    phases = steps // PHASE
    groups = width // 8
    scale = DT ** 0.5

    row_id, col_id, core_id = lax.axis_index("row"), lax.axis_index("col"), lax.axis_index("core")
    up, down = lax.rem(row_id + row_size - 1, row_size), lax.rem(row_id + 1, row_size)
    flat = col_id * core_size + core_id
    total = col_size * core_size
    lflat, rflat = lax.rem(flat + total - 1, total), lax.rem(flat + 1, total)
    above, below = {"row": up}, {"row": down}
    left = {"col": lax.div(lflat, core_size), "core": lax.rem(lflat, core_size)}
    right = {"col": lax.div(rflat, core_size), "core": lax.rem(rflat, core_size)}

    barrier = pltpu.get_barrier_semaphore()
    for dev in (above, below, left, right):
        pl.semaphore_signal(barrier, inc=1, device_id=dev, device_id_type=MESH)

    srcs = (u_hbm, f_hbm, w_hbm)
    cblocks = width // LANES

    def fetch(k):
        dep = halo if k < 2 else half

        def part(n, first, count):
            return [pltpu.make_async_copy(
                srcs[k].at[pl.ds(first, count), pl.ds(cb * LANES, LANES)],
                nat.at[k, cb, pl.ds(halo + first, count), :], loc_sem.at[k, cb, n]) for cb in range(cblocks)]
        return part(0, 0, dep) + part(1, rows - dep, dep), part(2, dep, rows - 2 * dep)

    local = [fetch(k) for k in range(3)]
    for copy in local[0][0] + local[0][1]:
        copy.start()
    params = [pltpu.make_async_copy(wts_hbm, wts_ref, par_sem.at[0]),
              pltpu.make_async_copy(gains_hbm, gains_ref, par_sem.at[1])]
    for copy in params:
        copy.start()
    for k in (1, 2):
        for copy in local[k][0] + local[k][1]:
            copy.start()
    pl.semaphore_wait(barrier, 4)

    def row_copies(k):
        dep = halo if k < 2 else half
        strip = lambda first: nat.at[k, :, pl.ds(first, dep), :]
        return [
            pltpu.make_async_remote_copy(strip(halo), strip(halo + rows), row_send.at[k, 0], row_recv.at[k, 0],
                                         device_id=above, device_id_type=MESH),
            pltpu.make_async_remote_copy(strip(halo + rows - dep), strip(halo - dep), row_send.at[k, 1],
                                         row_recv.at[k, 1], device_id=below, device_id_type=MESH),
        ]

    def col_copies(ref, dep, send, recv):
        return [
            pltpu.make_async_remote_copy(ref.at[:, pl.ds(org, dep), :], ref.at[:, pl.ds(org + width, dep), :],
                                         send.at[0], recv.at[0], device_id=left, device_id_type=MESH),
            pltpu.make_async_remote_copy(ref.at[:, pl.ds(org + width - dep, dep), :], ref.at[:, pl.ds(org - dep, dep), :],
                                         send.at[1], recv.at[1], device_id=right, device_id_type=MESH),
        ]

    rcopies = [row_copies(k) for k in range(3)]
    for k in range(3):
        for copy in local[k][0]:
            copy.wait()
        for copy in rcopies[k]:
            copy.start()
    for copy in params:
        copy.wait()

    def arrive(k, dst, factor):
        for copy in local[k][1] + rcopies[k]:
            copy.wait()
        for cb in range(cblocks):
            for b in range(nb):
                val = jnp.transpose(nat[k, cb, pl.ds(b, LANES, stride=nb), :])
                if factor is not None:
                    val = val * factor
                dst[b, pl.ds(org + cb * LANES, LANES), :] = val

    def depart(src, k, out, factor):
        for cb in range(cblocks):
            for b in range(nb):
                val = jnp.transpose(src[b, pl.ds(org + cb * LANES, LANES), :])
                if factor is not None:
                    val = val * factor
                nat[k, cb, pl.ds(b, LANES, stride=nb), :] = val
            out[:, pl.ds(cb * LANES, LANES)] = nat[k, cb, pl.ds(halo, rows), :]

    arrive(0, ubase.at[0], scale)
    for copy in col_copies(ubase.at[0], fdep, u_send.at[0], u_recv.at[0]):
        copy.start()
    wts = [[wts_ref[i, j] for j in range(3)] for i in range(3)]
    flip = [[wts_ref[2 - i, 2 - j] for j in range(3)] for i in range(3)]
    mid_wt = wts_ref[1, 1] + DT

    def sweep(body, base, count):
        for off in range(0, count, 8 * UNROLL):
            body(base + off, min(8 * UNROLL, count - off))

    def cover(step_body, dep, ahead):
        mark = width // 4 + 1

        def early():
            sweep(functools.partial(step_body, 1), org + mark, ahead)

        def first():
            sweep(functools.partial(step_body, 1), org + 1, mark - 1)
            sweep(functools.partial(step_body, 1), org + mark + ahead, width - 1 - mark - ahead)

        def middle():
            for j in range(2, PHASE + 1):
                sweep(functools.partial(step_body, j), org + j, width - 2 * j)

        def sides():
            for j in range(1, PHASE):
                sweep(functools.partial(step_body, j), org + j - dep, dep)
                sweep(functools.partial(step_body, j), org + width - j, dep)
            sweep(functools.partial(step_body, PHASE), org, PHASE)
            sweep(functools.partial(step_body, PHASE), org + width - PHASE, PHASE)
        return early, first, middle, sides

    def level(base, par, j):
        if j == 0:
            return base.at[par * BANKED]
        return base.at[(1 - par) * BANKED] if j == PHASE else inner.at[j - 1]

    def reaction(val, t, b, at):
        sq = val * val
        weight = mid_wt - sq
        coef[t, b, at, :] = (weight - sq) - sq
        return weight

    def fwd_body(phase, forced, j, base, cols):
        par = phase % 2 if isinstance(phase, int) else lax.rem(phase, 2)
        src, dst, t = level(ubase, par, j - 1), level(ubase, par, j), phase * PHASE + (j - 1)
        at = pl.ds(base, cols)
        sums = stencil_blocks(lambda b, d: src[b, pl.ds(base + d, cols), :], wts,
                              lambda b, mid: reaction(mid, t, b, at), nb)
        for b in range(nb):
            dst[b, at, :] = sums[b] + gains_ref[t] * force[b, at, :] if forced else sums[b]

    sweep(functools.partial(fwd_body, 0, False, 1), org + 1, width - 2)
    arrive(1, force, scale)
    fcopies = col_copies(force, fdep, f_send, f_recv)
    for copy in fcopies:
        copy.start()

    for b in range(nb):
        at = pl.ds(org + 1, width - 2)
        inner[0, b, at, :] = inner[0, b, at, :] + gains_ref[0] * force[b, at, :]

    def adj_body(phase, j, base, cols):
        par = phase % 2 if isinstance(phase, int) else lax.rem(phase, 2)
        src, dst, t = level(lbase, par, j - 1), level(lbase, par, j), steps - (phase * PHASE + j)
        gain = gains_ref[t]
        at = pl.ds(base, cols)

        def centre(b, mid):
            acc[b, at, :] += gain * mid
            return coef[t, b, at, :]
        sums = stencil_blocks(lambda b, d: src[b, pl.ds(base + d, cols), :], flip, centre, nb)
        for b in range(nb):
            dst[b, at, :] = sums[b]

    def adj_sweeps(phase):
        return cover(functools.partial(adj_body, phase), adep, width // 2)

    def l_strips(phase):
        par = phase % 2 if isinstance(phase, int) else lax.rem(phase, 2)
        return col_copies(lbase.at[par * BANKED], adep, l_send.at[par], l_recv.at[par])

    def adj_turn(phase, _):
        for copy in l_strips(phase):
            copy.wait()
        early, first, middle, _ = adj_sweeps(phase + 1)
        early()
        adj_sweeps(phase)[3]()
        for copy in l_strips(phase + 1):
            copy.start()
        first()
        middle()
        return 0

    def fwd_sweeps(phase):
        return cover(functools.partial(fwd_body, phase, True), fdep, width // 4)

    def u_strips(phase):
        par = phase % 2 if isinstance(phase, int) else lax.rem(phase, 2)
        return col_copies(ubase.at[par * BANKED], fdep, u_send.at[par], u_recv.at[par])

    def fwd_close(phase):
        fwd_sweeps(phase)[3]()
        last = phase * PHASE + (PHASE - 1)
        for at in (pl.ds(org - PHASE, PHASE), pl.ds(org + width, PHASE)):
            for b in range(nb):
                reaction(inner[PHASE - 2, b, at, :], last, b, at)

    def fwd_turn(phase, _):
        for copy in u_strips(phase):
            copy.wait()

        @pl.when(phase == 0)
        def _():
            for copy in fcopies:
                copy.wait()
        early, first, middle, _ = fwd_sweeps(phase + 1)
        early()
        fwd_close(phase)
        for copy in u_strips(phase + 1):
            copy.start()
        first()
        middle()
        return 0

    fwd_sweeps(0)[2]()
    lax.fori_loop(0, phases - 1, fwd_turn, 0)

    arrive(2, lbase.at[0], None)
    for copy in l_strips(0):
        copy.start()
    acc[...] = jnp.zeros(acc.shape, jnp.float32)
    for copy in u_strips(phases - 1):
        copy.wait()
    early, first, middle, _ = adj_sweeps(0)
    early()
    fwd_close(phases - 1)
    first()
    middle()
    depart(ubase.at[phases % 2 * BANKED], 0, uo_ref, 1.0 / scale)
    lax.fori_loop(0, phases - 1, adj_turn, 0)
    for copy in l_strips(phases - 1):
        copy.wait()
    adj_sweeps(phases - 1)[3]()
    lo_ref[...] = lbase[phases % 2 * BANKED, :, pl.ds(org, width), :]


def unlane(tiles, org, u_ref, l_ref, a_ref, uo_hbm, go_hbm, gf_hbm, nat, sem):
    rows, width = tiles
    nb = l_ref.shape[0]
    halo = (nb * LANES - rows) // 2
    copies = [pltpu.make_async_copy(u_ref, uo_hbm, sem.at[0, 0])]
    copies[0].start()
    for k, (src, first, out) in enumerate(((l_ref, 0, go_hbm), (a_ref, org, gf_hbm))):
        for cb in range(width // LANES):
            for b in range(nb):
                nat[k, cb, pl.ds(b, LANES, stride=nb), :] = jnp.transpose(src[b, pl.ds(first + cb * LANES, LANES), :])
            copies.append(pltpu.make_async_copy(nat.at[k, cb, pl.ds(halo, rows), :],
                                                out.at[:, pl.ds(cb * LANES, LANES)], sem.at[k + 1, cb]))
            copies[-1].start()
    for copy in copies:
        copy.wait()


def solution(mesh):
    row_size, col_size, core_size = mesh.shape["row"], mesh.shape["col"], mesh.shape["core"]
    field_spec = P(("mem", "row"), ("col", "core"))

    def local_run(u_init, forcing, loss_weight, weights, gains):
        rows, width = u_init.shape
        steps = gains.shape[0]
        nb = -(-(rows + 4 * steps) // LANES)
        cols = width + 4 * PHASE + 8
        cblocks = width // LANES
        f32 = jnp.float32
        field = (nb, cols, LANES)
        dma = pltpu.SemaphoreType.DMA
        hbm, vmem = pl.BlockSpec(memory_space=pl.ANY), pl.BlockSpec(memory_space=pltpu.VMEM)
        lanes_out = pl.pallas_call(
            functools.partial(kernel, row_size, col_size, core_size, (rows, width, steps)),
            out_shape=[jax.ShapeDtypeStruct(dims, f32) for dims in ((rows, width), (nb, width, LANES), field)],
            in_specs=[hbm] * 5,
            out_specs=[vmem, vmem, vmem],
            scratch_shapes=[
                pltpu.SMEM(weights.shape, f32),
                pltpu.SMEM(gains.shape, f32),
                pltpu.VMEM((3, cblocks, nb * LANES, LANES), f32),
                pltpu.VMEM((2 * BANKED,) + field, f32),
                pltpu.VMEM((2 * BANKED,) + field, f32),
                pltpu.VMEM((PHASE,) + field, f32),
                pltpu.VMEM((steps,) + field, f32),
                pltpu.VMEM((BANKED,) + field, f32),
                dma((2,)),
                dma((3, cblocks, 3)),
                dma((3, 2)),
                dma((3, 2)),
                dma((2,)),
                dma((2,)),
                dma((2, 2)),
                dma((2, 2)),
                dma((2, 2)),
                dma((2, 2)),
            ],
            compiler_params=pltpu.CompilerParams(
                collective_id=0, has_side_effects=True, vmem_limit_bytes=52 * 1024 * 1024),
            name="steps",
        )(*(pltpu.with_memory_space_constraint(x, pltpu.HBM) for x in (weights, gains, u_init, forcing, loss_weight)))
        return pl.pallas_call(
            functools.partial(unlane, (rows, width), 2 * PHASE),
            out_shape=[jax.ShapeDtypeStruct((rows, width), f32)] * 3,
            in_specs=[vmem] * 3,
            out_specs=[hbm] * 3,
            scratch_shapes=[pltpu.VMEM((2, cblocks, nb * LANES, LANES), f32), dma((3, 2))],
            compiler_params=pltpu.CompilerParams(vmem_limit_bytes=16 * 1024 * 1024),
            name="unlane",
        )(*(pltpu.with_memory_space_constraint(x, pltpu.VMEM) for x in lanes_out))

    return jax.shard_map(local_run, mesh=mesh, in_specs=(field_spec, field_spec, field_spec, P(), P()),
                         out_specs=(field_spec, field_spec, field_spec), check_vma=False)
```

```python
import functools

import jax
import jax.numpy as jnp
from jax import lax
from jax.experimental import pallas as pl
from jax.experimental.pallas import tpu as pltpu
from jax.sharding import PartitionSpec as P


DT = 0.01
LANES = 128
PHASE = 8
BANKED = 4
UNROLL = 32
MESH = pl.DeviceIdType.MESH


def stencil_blocks(load, wts, centre, nb):
    part = {}
    for b in range(nb):
        left, mid, right = load(b, -1), load(b, 0), load(b, 1)
        part[b, -1] = (wts[0][0] * left + wts[0][1] * mid) + wts[0][2] * right
        part[b, 0] = (wts[1][0] * left + centre(b, mid) * mid) + wts[1][2] * right
        part[b, 1] = (wts[2][0] * left + wts[2][1] * mid) + wts[2][2] * right
    part[-1, -1] = pltpu.roll(part[nb - 1, -1], 1, 1)
    part[nb, 1] = pltpu.roll(part[0, 1], LANES - 1, 1)
    return [(part[b - 1, -1] + part[b, 0]) + part[b + 1, 1] for b in range(nb)]


def kernel(row_size, col_size, core_size, tiles, wts_hbm, gains_hbm, u_hbm, f_hbm, w_hbm, uo_ref, lo_ref, ao_ref,
           wts_ref, gains_ref, nat, ubase, lbase, inner, coef, forces, par_sem, loc_sem, row_send, row_recv, f_send, f_recv,
           u_send, u_recv, l_send, l_recv):
    rows, width, steps = tiles
    force, acc = forces.at[0], ao_ref
    nb = force.shape[0]
    halo = (nb * LANES - rows) // 2
    half = halo // 2
    fdep, adep = 2 * PHASE, PHASE
    org = fdep
    phases = steps // PHASE
    groups = width // 8
    scale = DT ** 0.5

    row_id, col_id, core_id = lax.axis_index("row"), lax.axis_index("col"), lax.axis_index("core")
    up, down = lax.rem(row_id + row_size - 1, row_size), lax.rem(row_id + 1, row_size)
    flat = col_id * core_size + core_id
    total = col_size * core_size
    lflat, rflat = lax.rem(flat + total - 1, total), lax.rem(flat + 1, total)
    above, below = {"row": up}, {"row": down}
    left = {"col": lax.div(lflat, core_size), "core": lax.rem(lflat, core_size)}
    right = {"col": lax.div(rflat, core_size), "core": lax.rem(rflat, core_size)}

    barrier = pltpu.get_barrier_semaphore()
    for dev in (above, below, left, right):
        pl.semaphore_signal(barrier, inc=1, device_id=dev, device_id_type=MESH)

    srcs = (u_hbm, f_hbm, w_hbm)
    cblocks = width // LANES

    def fetch(k):
        dep = halo if k < 2 else half

        def part(n, first, count):
            return [pltpu.make_async_copy(
                srcs[k].at[pl.ds(first, count), pl.ds(cb * LANES, LANES)],
                nat.at[k, cb, pl.ds(halo + first, count), :], loc_sem.at[k, cb, n]) for cb in range(cblocks)]
        return part(0, 0, dep) + part(1, rows - dep, dep), part(2, dep, rows - 2 * dep)

    local = [fetch(k) for k in range(3)]
    for copy in local[0][0] + local[0][1]:
        copy.start()
    params = [pltpu.make_async_copy(wts_hbm, wts_ref, par_sem.at[0]),
              pltpu.make_async_copy(gains_hbm, gains_ref, par_sem.at[1])]
    for copy in params:
        copy.start()
    for k in (1, 2):
        for copy in local[k][0] + local[k][1]:
            copy.start()
    pl.semaphore_wait(barrier, 4)

    def row_copies(k):
        dep = halo if k < 2 else half
        strip = lambda first: nat.at[k, :, pl.ds(first, dep), :]
        return [
            pltpu.make_async_remote_copy(strip(halo), strip(halo + rows), row_send.at[k, 0], row_recv.at[k, 0],
                                         device_id=above, device_id_type=MESH),
            pltpu.make_async_remote_copy(strip(halo + rows - dep), strip(halo - dep), row_send.at[k, 1],
                                         row_recv.at[k, 1], device_id=below, device_id_type=MESH),
        ]

    def col_copies(ref, dep, send, recv):
        return [
            pltpu.make_async_remote_copy(ref.at[:, pl.ds(org, dep), :], ref.at[:, pl.ds(org + width, dep), :],
                                         send.at[0], recv.at[0], device_id=left, device_id_type=MESH),
            pltpu.make_async_remote_copy(ref.at[:, pl.ds(org + width - dep, dep), :], ref.at[:, pl.ds(org - dep, dep), :],
                                         send.at[1], recv.at[1], device_id=right, device_id_type=MESH),
        ]

    rcopies = [row_copies(k) for k in range(3)]
    for k in range(3):
        for copy in local[k][0]:
            copy.wait()
        for copy in rcopies[k]:
            copy.start()
    for copy in params:
        copy.wait()

    def arrive(k, dst, factor):
        for copy in local[k][1] + rcopies[k]:
            copy.wait()
        for cb in range(cblocks):
            for b in range(nb):
                val = jnp.transpose(nat[k, cb, pl.ds(b, LANES, stride=nb), :])
                if factor is not None:
                    val = val * factor
                dst[b, pl.ds(org + cb * LANES, LANES), :] = val

    def depart(src, k, out, factor):
        for cb in range(cblocks):
            for b in range(nb):
                val = jnp.transpose(src[b, pl.ds(org + cb * LANES, LANES), :])
                if factor is not None:
                    val = val * factor
                nat[k, cb, pl.ds(b, LANES, stride=nb), :] = val
            out[:, pl.ds(cb * LANES, LANES)] = nat[k, cb, pl.ds(halo, rows), :]

    arrive(0, ubase.at[0], scale)
    for copy in col_copies(ubase.at[0], fdep, u_send.at[0], u_recv.at[0]):
        copy.start()
    wts = [[wts_ref[i, j] for j in range(3)] for i in range(3)]
    flip = [[wts_ref[2 - i, 2 - j] for j in range(3)] for i in range(3)]
    mid_wt = wts_ref[1, 1] + DT

    def sweep(body, base, count):
        for off in range(0, count, 8 * UNROLL):
            body(base + off, min(8 * UNROLL, count - off))

    def cover(step_body, dep, ahead):
        mark = width // 4 + 1

        def early():
            sweep(functools.partial(step_body, 1), org + mark, ahead)

        def first():
            sweep(functools.partial(step_body, 1), org + 1, mark - 1)
            sweep(functools.partial(step_body, 1), org + mark + ahead, width - 1 - mark - ahead)

        def middle():
            for j in range(2, PHASE + 1):
                sweep(functools.partial(step_body, j), org + j, width - 2 * j)

        def sides():
            for j in range(1, PHASE):
                sweep(functools.partial(step_body, j), org + j - dep, dep)
                sweep(functools.partial(step_body, j), org + width - j, dep)
            sweep(functools.partial(step_body, PHASE), org, PHASE)
            sweep(functools.partial(step_body, PHASE), org + width - PHASE, PHASE)
        return early, first, middle, sides

    def level(base, par, j):
        if j == 0:
            return base.at[par * BANKED]
        return base.at[(1 - par) * BANKED] if j == PHASE else inner.at[j - 1]

    def reaction(val, t, b, at):
        sq = val * val
        weight = mid_wt - sq
        coef[t, b, at, :] = (weight - sq) - sq
        return weight

    def fwd_body(phase, forced, j, base, cols):
        par = phase % 2 if isinstance(phase, int) else lax.rem(phase, 2)
        src, dst, t = level(ubase, par, j - 1), level(ubase, par, j), phase * PHASE + (j - 1)
        at = pl.ds(base, cols)
        sums = stencil_blocks(lambda b, d: src[b, pl.ds(base + d, cols), :], wts,
                              lambda b, mid: reaction(mid, t, b, at), nb)
        for b in range(nb):
            dst[b, at, :] = sums[b] + gains_ref[t] * force[b, at, :] if forced else sums[b]

    sweep(functools.partial(fwd_body, 0, False, 1), org + 1, width - 2)
    arrive(1, force, scale)
    fcopies = col_copies(force, fdep, f_send, f_recv)
    for copy in fcopies:
        copy.start()

    for b in range(nb):
        at = pl.ds(org + 1, width - 2)
        inner[0, b, at, :] = inner[0, b, at, :] + gains_ref[0] * force[b, at, :]

    def adj_body(phase, j, base, cols):
        par = phase % 2 if isinstance(phase, int) else lax.rem(phase, 2)
        src, dst, t = level(lbase, par, j - 1), level(lbase, par, j), steps - (phase * PHASE + j)
        gain = gains_ref[t]
        at = pl.ds(base, cols)

        def centre(b, mid):
            if isinstance(phase, int) and phase == 0 and j == 1:
                acc[b, at, :] = gain * mid
            else:
                acc[b, at, :] += gain * mid
            return coef[t, b, at, :]
        sums = stencil_blocks(lambda b, d: src[b, pl.ds(base + d, cols), :], flip, centre, nb)
        for b in range(nb):
            dst[b, at, :] = sums[b]

    def adj_sweeps(phase):
        return cover(functools.partial(adj_body, phase), adep, width * 5 // 8)

    def l_strips(phase):
        par = phase % 2 if isinstance(phase, int) else lax.rem(phase, 2)
        return col_copies(lbase.at[par * BANKED], adep, l_send.at[par], l_recv.at[par])

    def adj_turn(phase, _):
        for copy in l_strips(phase):
            copy.wait()
        early, first, middle, _ = adj_sweeps(phase + 1)
        early()
        adj_sweeps(phase)[3]()
        for copy in l_strips(phase + 1):
            copy.start()
        first()
        middle()
        return 0

    def fwd_sweeps(phase):
        return cover(functools.partial(fwd_body, phase, True), fdep, width // 4)

    def u_strips(phase):
        par = phase % 2 if isinstance(phase, int) else lax.rem(phase, 2)
        return col_copies(ubase.at[par * BANKED], fdep, u_send.at[par], u_recv.at[par])

    def fwd_close(phase):
        fwd_sweeps(phase)[3]()
        last = phase * PHASE + (PHASE - 1)
        for at in (pl.ds(org - PHASE, PHASE), pl.ds(org + width, PHASE)):
            for b in range(nb):
                reaction(inner[PHASE - 2, b, at, :], last, b, at)

    def fwd_turn(phase, _):
        for copy in u_strips(phase):
            copy.wait()

        @pl.when(phase == 0)
        def _():
            for copy in fcopies:
                copy.wait()
        early, first, middle, _ = fwd_sweeps(phase + 1)
        early()
        fwd_close(phase)
        for copy in u_strips(phase + 1):
            copy.start()
        first()
        middle()
        return 0

    fwd_sweeps(0)[2]()
    lax.fori_loop(0, phases - 1, fwd_turn, 0)

    arrive(2, lbase.at[0], None)
    for copy in l_strips(0):
        copy.start()
    for at in (pl.ds(0, org + 8), pl.ds(org + width - 8, org + 8)):
        acc[:, at, :] = jnp.zeros((nb, org + 8, LANES), jnp.float32)
    for copy in u_strips(phases - 1):
        copy.wait()
    early, first, middle, _ = adj_sweeps(0)
    early()
    fwd_close(phases - 1)
    first()
    middle()
    lax.fori_loop(0, phases - 1, adj_turn, 0)
    inside = width - 2 * PHASE
    lo_ref[:, pl.ds(PHASE, inside), :] = lbase[phases % 2 * BANKED, :, pl.ds(org + PHASE, inside), :]
    for copy in l_strips(phases - 1):
        copy.wait()
    depart(ubase.at[phases % 2 * BANKED], 0, uo_ref, 1.0 / scale)
    adj_sweeps(phases - 1)[3]()
    for edge in (0, width - PHASE):
        lo_ref[:, pl.ds(edge, PHASE), :] = lbase[phases % 2 * BANKED, :, pl.ds(org + edge, PHASE), :]


def unlane(tiles, org, u_ref, l_ref, a_ref, uo_hbm, go_hbm, gf_hbm, nat, sem):
    rows, width = tiles
    nb = l_ref.shape[0]
    halo = (nb * LANES - rows) // 2
    copies = [pltpu.make_async_copy(u_ref, uo_hbm, sem.at[0, 0])]
    copies[0].start()
    for k, (src, first, out) in enumerate(((l_ref, 0, go_hbm), (a_ref, org, gf_hbm))):
        for cb in range(width // LANES):
            for b in range(nb):
                nat[k, cb, pl.ds(b, LANES, stride=nb), :] = jnp.transpose(src[b, pl.ds(first + cb * LANES, LANES), :])
            copies.append(pltpu.make_async_copy(nat.at[k, cb, pl.ds(halo, rows), :],
                                                out.at[:, pl.ds(cb * LANES, LANES)], sem.at[k + 1, cb]))
            copies[-1].start()
    for copy in copies:
        copy.wait()


def solution(mesh):
    row_size, col_size, core_size = mesh.shape["row"], mesh.shape["col"], mesh.shape["core"]
    field_spec = P(("mem", "row"), ("col", "core"))

    def local_run(u_init, forcing, loss_weight, weights, gains):
        rows, width = u_init.shape
        steps = gains.shape[0]
        nb = -(-(rows + 4 * steps) // LANES)
        cols = width + 4 * PHASE + 8
        cblocks = width // LANES
        f32 = jnp.float32
        field = (nb, cols, LANES)
        dma = pltpu.SemaphoreType.DMA
        hbm, vmem = pl.BlockSpec(memory_space=pl.ANY), pl.BlockSpec(memory_space=pltpu.VMEM)
        lanes_out = pl.pallas_call(
            functools.partial(kernel, row_size, col_size, core_size, (rows, width, steps)),
            out_shape=[jax.ShapeDtypeStruct(dims, f32) for dims in ((rows, width), (nb, width, LANES), field)],
            in_specs=[hbm] * 5,
            out_specs=[vmem, vmem, vmem],
            scratch_shapes=[
                pltpu.SMEM(weights.shape, f32),
                pltpu.SMEM(gains.shape, f32),
                pltpu.VMEM((3, cblocks, nb * LANES, LANES), f32),
                pltpu.VMEM((2 * BANKED,) + field, f32),
                pltpu.VMEM((2 * BANKED,) + field, f32),
                pltpu.VMEM((PHASE,) + field, f32),
                pltpu.VMEM((steps,) + field, f32),
                pltpu.VMEM((BANKED,) + field, f32),
                dma((2,)),
                dma((3, cblocks, 3)),
                dma((3, 2)),
                dma((3, 2)),
                dma((2,)),
                dma((2,)),
                dma((2, 2)),
                dma((2, 2)),
                dma((2, 2)),
                dma((2, 2)),
            ],
            compiler_params=pltpu.CompilerParams(
                collective_id=0, has_side_effects=True, vmem_limit_bytes=52 * 1024 * 1024),
            name="steps",
        )(*(pltpu.with_memory_space_constraint(x, pltpu.HBM) for x in (weights, gains, u_init, forcing, loss_weight)))
        return pl.pallas_call(
            functools.partial(unlane, (rows, width), 2 * PHASE),
            out_shape=[jax.ShapeDtypeStruct((rows, width), f32)] * 3,
            in_specs=[vmem] * 3,
            out_specs=[hbm] * 3,
            scratch_shapes=[pltpu.VMEM((2, cblocks, nb * LANES, LANES), f32), dma((3, 2))],
            compiler_params=pltpu.CompilerParams(vmem_limit_bytes=16 * 1024 * 1024),
            name="unlane",
        )(*(pltpu.with_memory_space_constraint(x, pltpu.VMEM) for x in lanes_out))

    return jax.shard_map(local_run, mesh=mesh, in_specs=(field_spec, field_spec, field_spec, P(), P()),
                         out_specs=(field_spec, field_spec, field_spec), check_vma=False)
```

```python
import functools

import jax
import jax.numpy as jnp
from jax import lax
from jax.experimental import pallas as pl
from jax.experimental.pallas import tpu as pltpu
from jax.sharding import PartitionSpec as P


DT = 0.01
LANES = 128
PHASE = 8
BANKED = 4
UNROLL = 32
MESH = pl.DeviceIdType.MESH


def stencil_blocks(load, wts, centre, nb):
    part = {}
    for b in range(nb):
        left, mid, right = load(b, -1), load(b, 0), load(b, 1)
        part[b, -1] = (wts[0][0] * left + wts[0][1] * mid) + wts[0][2] * right
        part[b, 0] = (wts[1][0] * left + centre(b, mid) * mid) + wts[1][2] * right
        part[b, 1] = (wts[2][0] * left + wts[2][1] * mid) + wts[2][2] * right
    part[-1, -1] = pltpu.roll(part[nb - 1, -1], 1, 1)
    part[nb, 1] = pltpu.roll(part[0, 1], LANES - 1, 1)
    return [(part[b - 1, -1] + part[b, 0]) + part[b + 1, 1] for b in range(nb)]


def kernel(row_size, col_size, core_size, tiles, wts_hbm, gains_hbm, u_hbm, f_hbm, w_hbm, uo_ref, lo_ref, ao_ref,
           wts_ref, gains_ref, nat, ubase, lbase, inner, coef, forces, par_sem, loc_sem, row_send, row_recv, f_send, f_recv,
           u_send, u_recv, l_send, l_recv):
    rows, width, steps = tiles
    force, acc = forces.at[0], ao_ref
    nb = force.shape[0]
    halo = (nb * LANES - rows) // 2
    half = halo // 2
    fdep, adep = 2 * PHASE, PHASE
    org = fdep
    phases = steps // PHASE
    groups = width // 8
    scale = DT ** 0.5

    row_id, col_id, core_id = lax.axis_index("row"), lax.axis_index("col"), lax.axis_index("core")
    up, down = lax.rem(row_id + row_size - 1, row_size), lax.rem(row_id + 1, row_size)
    flat = col_id * core_size + core_id
    total = col_size * core_size
    lflat, rflat = lax.rem(flat + total - 1, total), lax.rem(flat + 1, total)
    above, below = {"row": up}, {"row": down}
    left = {"col": lax.div(lflat, core_size), "core": lax.rem(lflat, core_size)}
    right = {"col": lax.div(rflat, core_size), "core": lax.rem(rflat, core_size)}

    barrier = pltpu.get_barrier_semaphore()
    for dev in (above, below, left, right):
        pl.semaphore_signal(barrier, inc=1, device_id=dev, device_id_type=MESH)

    srcs = (u_hbm, f_hbm, w_hbm)
    cblocks = width // LANES

    def fetch(k):
        dep = halo if k < 2 else half

        def part(n, first, count):
            return [pltpu.make_async_copy(
                srcs[k].at[pl.ds(first, count), pl.ds(cb * LANES, LANES)],
                nat.at[k, cb, pl.ds(halo + first, count), :], loc_sem.at[k, cb, n]) for cb in range(cblocks)]
        return part(0, 0, dep) + part(1, rows - dep, dep), part(2, dep, rows - 2 * dep)

    local = [fetch(k) for k in range(3)]
    for copy in local[0][0] + local[0][1]:
        copy.start()
    params = [pltpu.make_async_copy(wts_hbm, wts_ref, par_sem.at[0]),
              pltpu.make_async_copy(gains_hbm, gains_ref, par_sem.at[1])]
    for copy in params:
        copy.start()
    for k in (1, 2):
        for copy in local[k][0] + local[k][1]:
            copy.start()
    pl.semaphore_wait(barrier, 4)

    def row_copies(k):
        dep = halo if k < 2 else half
        strip = lambda first: nat.at[k, :, pl.ds(first, dep), :]
        return [
            pltpu.make_async_remote_copy(strip(halo), strip(halo + rows), row_send.at[k, 0], row_recv.at[k, 0],
                                         device_id=above, device_id_type=MESH),
            pltpu.make_async_remote_copy(strip(halo + rows - dep), strip(halo - dep), row_send.at[k, 1],
                                         row_recv.at[k, 1], device_id=below, device_id_type=MESH),
        ]

    def col_copies(ref, dep, send, recv):
        return [
            pltpu.make_async_remote_copy(ref.at[:, pl.ds(org, dep), :], ref.at[:, pl.ds(org + width, dep), :],
                                         send.at[0], recv.at[0], device_id=left, device_id_type=MESH),
            pltpu.make_async_remote_copy(ref.at[:, pl.ds(org + width - dep, dep), :], ref.at[:, pl.ds(org - dep, dep), :],
                                         send.at[1], recv.at[1], device_id=right, device_id_type=MESH),
        ]

    rcopies = [row_copies(k) for k in range(3)]
    for k in range(3):
        for copy in local[k][0]:
            copy.wait()
        for copy in rcopies[k]:
            copy.start()
    for copy in params:
        copy.wait()

    def arrive(k, dst, factor):
        for copy in local[k][1] + rcopies[k]:
            copy.wait()
        for cb in range(cblocks):
            for b in range(nb):
                val = jnp.transpose(nat[k, cb, pl.ds(b, LANES, stride=nb), :])
                if factor is not None:
                    val = val * factor
                dst[b, pl.ds(org + cb * LANES, LANES), :] = val

    def depart(src, k, out, factor):
        for cb in range(cblocks):
            for b in range(nb):
                val = jnp.transpose(src[b, pl.ds(org + cb * LANES, LANES), :])
                if factor is not None:
                    val = val * factor
                nat[k, cb, pl.ds(b, LANES, stride=nb), :] = val
            out[:, pl.ds(cb * LANES, LANES)] = nat[k, cb, pl.ds(halo, rows), :]

    arrive(0, ubase.at[0], scale)
    for copy in col_copies(ubase.at[0], fdep, u_send.at[0], u_recv.at[0]):
        copy.start()
    wts = [[wts_ref[i, j] for j in range(3)] for i in range(3)]
    flip = [[wts_ref[2 - i, 2 - j] for j in range(3)] for i in range(3)]
    mid_wt = wts_ref[1, 1] + DT

    def sweep(body, base, count):
        for off in range(0, count, 8 * UNROLL):
            body(base + off, min(8 * UNROLL, count - off))

    def cover(step_body, dep, ahead):
        mark = width // 4 + 1

        def early():
            sweep(functools.partial(step_body, 1), org + mark, ahead)

        def first():
            sweep(functools.partial(step_body, 1), org + 1, mark - 1)
            sweep(functools.partial(step_body, 1), org + mark + ahead, width - 1 - mark - ahead)

        def middle():
            for j in range(2, PHASE + 1):
                sweep(functools.partial(step_body, j), org + j, width - 2 * j)

        def sides():
            for j in range(1, PHASE):
                sweep(functools.partial(step_body, j), org + j - dep, dep)
                sweep(functools.partial(step_body, j), org + width - j, dep)
            sweep(functools.partial(step_body, PHASE), org, PHASE)
            sweep(functools.partial(step_body, PHASE), org + width - PHASE, PHASE)
        return early, first, middle, sides

    def level(base, par, j):
        if j == 0:
            return base.at[par * BANKED]
        return base.at[(1 - par) * BANKED] if j == PHASE else inner.at[j - 1]

    def reaction(val, t, b, at):
        weight = mid_wt - val * val
        coef[t, b, at, :] = weight
        return weight

    def fwd_body(phase, forced, j, base, cols):
        par = phase % 2 if isinstance(phase, int) else lax.rem(phase, 2)
        src, dst, t = level(ubase, par, j - 1), level(ubase, par, j), phase * PHASE + (j - 1)
        at = pl.ds(base, cols)
        sums = stencil_blocks(lambda b, d: src[b, pl.ds(base + d, cols), :], wts,
                              lambda b, mid: reaction(mid, t, b, at), nb)
        for b in range(nb):
            dst[b, at, :] = sums[b] + gains_ref[t] * force[b, at, :] if forced else sums[b]

    sweep(functools.partial(fwd_body, 0, False, 1), org + 1, width - 2)
    arrive(1, force, scale)
    fcopies = col_copies(force, fdep, f_send, f_recv)
    for copy in fcopies:
        copy.start()

    for b in range(nb):
        at = pl.ds(org + 1, width - 2)
        inner[0, b, at, :] = inner[0, b, at, :] + gains_ref[0] * force[b, at, :]

    def adj_body(phase, j, base, cols):
        par = phase % 2 if isinstance(phase, int) else lax.rem(phase, 2)
        src, dst, t = level(lbase, par, j - 1), level(lbase, par, j), steps - (phase * PHASE + j)
        gain = gains_ref[t]
        at = pl.ds(base, cols)

        def centre(b, mid):
            if isinstance(phase, int) and phase == 0 and j == 1:
                acc[b, at, :] = gain * mid
            else:
                acc[b, at, :] += gain * mid
            return 3.0 * coef[t, b, at, :] - 2.0 * mid_wt
        sums = stencil_blocks(lambda b, d: src[b, pl.ds(base + d, cols), :], flip, centre, nb)
        for b in range(nb):
            dst[b, at, :] = sums[b]

    def adj_sweeps(phase):
        return cover(functools.partial(adj_body, phase), adep, width * 5 // 8)

    def l_strips(phase):
        par = phase % 2 if isinstance(phase, int) else lax.rem(phase, 2)
        return col_copies(lbase.at[par * BANKED], adep, l_send.at[par], l_recv.at[par])

    def adj_turn(phase, _):
        for copy in l_strips(phase):
            copy.wait()
        early, first, middle, _ = adj_sweeps(phase + 1)
        early()
        adj_sweeps(phase)[3]()
        for copy in l_strips(phase + 1):
            copy.start()
        first()
        middle()
        return 0

    def fwd_sweeps(phase):
        return cover(functools.partial(fwd_body, phase, True), fdep, width // 4)

    def u_strips(phase):
        par = phase % 2 if isinstance(phase, int) else lax.rem(phase, 2)
        return col_copies(ubase.at[par * BANKED], fdep, u_send.at[par], u_recv.at[par])

    def fwd_close(phase):
        fwd_sweeps(phase)[3]()
        last = phase * PHASE + (PHASE - 1)
        for at in (pl.ds(org - PHASE, PHASE), pl.ds(org + width, PHASE)):
            for b in range(nb):
                reaction(inner[PHASE - 2, b, at, :], last, b, at)

    def fwd_turn(phase, _):
        for copy in u_strips(phase):
            copy.wait()

        @pl.when(phase == 0)
        def _():
            for copy in fcopies:
                copy.wait()
        early, first, middle, _ = fwd_sweeps(phase + 1)
        early()
        fwd_close(phase)
        for copy in u_strips(phase + 1):
            copy.start()
        first()
        middle()
        return 0

    fwd_sweeps(0)[2]()
    lax.fori_loop(0, phases - 1, fwd_turn, 0)

    arrive(2, lbase.at[0], None)
    for copy in l_strips(0):
        copy.start()
    for at in (pl.ds(0, org + 8), pl.ds(org + width - 8, org + 8)):
        acc[:, at, :] = jnp.zeros((nb, org + 8, LANES), jnp.float32)
    for copy in u_strips(phases - 1):
        copy.wait()
    early, first, middle, _ = adj_sweeps(0)
    early()
    fwd_close(phases - 1)
    first()
    middle()
    lax.fori_loop(0, phases - 1, adj_turn, 0)
    inside = width - 2 * PHASE
    lo_ref[:, pl.ds(PHASE, inside), :] = lbase[phases % 2 * BANKED, :, pl.ds(org + PHASE, inside), :]
    for copy in l_strips(phases - 1):
        copy.wait()
    depart(ubase.at[phases % 2 * BANKED], 0, uo_ref, 1.0 / scale)
    adj_sweeps(phases - 1)[3]()
    for edge in (0, width - PHASE):
        lo_ref[:, pl.ds(edge, PHASE), :] = lbase[phases % 2 * BANKED, :, pl.ds(org + edge, PHASE), :]


def unlane(tiles, org, u_ref, l_ref, a_ref, uo_hbm, go_hbm, gf_hbm, nat, sem):
    rows, width = tiles
    nb = l_ref.shape[0]
    halo = (nb * LANES - rows) // 2
    copies = [pltpu.make_async_copy(u_ref, uo_hbm, sem.at[0, 0])]
    copies[0].start()
    for k, (src, first, out) in enumerate(((l_ref, 0, go_hbm), (a_ref, org, gf_hbm))):
        for cb in range(width // LANES):
            for b in range(nb):
                nat[k, cb, pl.ds(b, LANES, stride=nb), :] = jnp.transpose(src[b, pl.ds(first + cb * LANES, LANES), :])
            copies.append(pltpu.make_async_copy(nat.at[k, cb, pl.ds(halo, rows), :],
                                                out.at[:, pl.ds(cb * LANES, LANES)], sem.at[k + 1, cb]))
            copies[-1].start()
    for copy in copies:
        copy.wait()


def solution(mesh):
    row_size, col_size, core_size = mesh.shape["row"], mesh.shape["col"], mesh.shape["core"]
    field_spec = P(("mem", "row"), ("col", "core"))

    def local_run(u_init, forcing, loss_weight, weights, gains):
        rows, width = u_init.shape
        steps = gains.shape[0]
        nb = -(-(rows + 4 * steps) // LANES)
        cols = width + 4 * PHASE + 8
        cblocks = width // LANES
        f32 = jnp.float32
        field = (nb, cols, LANES)
        dma = pltpu.SemaphoreType.DMA
        hbm, vmem = pl.BlockSpec(memory_space=pl.ANY), pl.BlockSpec(memory_space=pltpu.VMEM)
        lanes_out = pl.pallas_call(
            functools.partial(kernel, row_size, col_size, core_size, (rows, width, steps)),
            out_shape=[jax.ShapeDtypeStruct(dims, f32) for dims in ((rows, width), (nb, width, LANES), field)],
            in_specs=[hbm] * 5,
            out_specs=[vmem, vmem, vmem],
            scratch_shapes=[
                pltpu.SMEM(weights.shape, f32),
                pltpu.SMEM(gains.shape, f32),
                pltpu.VMEM((3, cblocks, nb * LANES, LANES), f32),
                pltpu.VMEM((2 * BANKED,) + field, f32),
                pltpu.VMEM((2 * BANKED,) + field, f32),
                pltpu.VMEM((PHASE,) + field, f32),
                pltpu.VMEM((steps,) + field, f32),
                pltpu.VMEM((BANKED,) + field, f32),
                dma((2,)),
                dma((3, cblocks, 3)),
                dma((3, 2)),
                dma((3, 2)),
                dma((2,)),
                dma((2,)),
                dma((2, 2)),
                dma((2, 2)),
                dma((2, 2)),
                dma((2, 2)),
            ],
            compiler_params=pltpu.CompilerParams(
                collective_id=0, has_side_effects=True, vmem_limit_bytes=52 * 1024 * 1024),
            name="steps",
        )(*(pltpu.with_memory_space_constraint(x, pltpu.HBM) for x in (weights, gains, u_init, forcing, loss_weight)))
        return pl.pallas_call(
            functools.partial(unlane, (rows, width), 2 * PHASE),
            out_shape=[jax.ShapeDtypeStruct((rows, width), f32)] * 3,
            in_specs=[vmem] * 3,
            out_specs=[hbm] * 3,
            scratch_shapes=[pltpu.VMEM((2, cblocks, nb * LANES, LANES), f32), dma((3, 2))],
            compiler_params=pltpu.CompilerParams(vmem_limit_bytes=16 * 1024 * 1024),
            name="unlane",
        )(*(pltpu.with_memory_space_constraint(x, pltpu.VMEM) for x in lanes_out))

    return jax.shard_map(local_run, mesh=mesh, in_specs=(field_spec, field_spec, field_spec, P(), P()),
                         out_specs=(field_spec, field_spec, field_spec), check_vma=False)
```

```python
import functools

import jax
import jax.numpy as jnp
from jax import lax
from jax.experimental import pallas as pl
from jax.experimental.pallas import tpu as pltpu
from jax.sharding import PartitionSpec as P


DT = 0.01
LANES = 128
PHASE = 8
BANKED = 4
UNROLL = 32
MESH = pl.DeviceIdType.MESH


def stencil_blocks(load, wts, centre, nb):
    part = {}
    for b in range(nb):
        left, mid, right = load(b, -1), load(b, 0), load(b, 1)
        part[b, -1] = (wts[0][0] * left + wts[0][1] * mid) + wts[0][2] * right
        part[b, 0] = (wts[1][0] * left + centre(b, mid) * mid) + wts[1][2] * right
        part[b, 1] = (wts[2][0] * left + wts[2][1] * mid) + wts[2][2] * right
    part[-1, -1] = pltpu.roll(part[nb - 1, -1], 1, 1)
    part[nb, 1] = pltpu.roll(part[0, 1], LANES - 1, 1)
    return [(part[b - 1, -1] + part[b, 0]) + part[b + 1, 1] for b in range(nb)]


def kernel(row_size, col_size, core_size, tiles, wts_hbm, gains_hbm, u_hbm, f_hbm, w_hbm, uo_ref, lo_ref, ao_ref,
           wts_ref, gains_ref, nat, ubase, lbase, inner, coef, forces, par_sem, loc_sem, row_send, row_recv, f_send, f_recv,
           u_send, u_recv, l_send, l_recv):
    rows, width, steps = tiles
    force, acc = forces.at[0], ao_ref
    nb = force.shape[0]
    halo = (nb * LANES - rows) // 2
    half = halo // 2
    fdep, adep = 2 * PHASE, PHASE
    org = fdep
    phases = steps // PHASE
    groups = width // 8
    scale = DT ** 0.5

    row_id, col_id, core_id = lax.axis_index("row"), lax.axis_index("col"), lax.axis_index("core")
    up, down = lax.rem(row_id + row_size - 1, row_size), lax.rem(row_id + 1, row_size)
    flat = col_id * core_size + core_id
    total = col_size * core_size
    lflat, rflat = lax.rem(flat + total - 1, total), lax.rem(flat + 1, total)
    above, below = {"row": up}, {"row": down}
    left = {"col": lax.div(lflat, core_size), "core": lax.rem(lflat, core_size)}
    right = {"col": lax.div(rflat, core_size), "core": lax.rem(rflat, core_size)}

    barrier = pltpu.get_barrier_semaphore()
    for dev in (above, below, left, right):
        pl.semaphore_signal(barrier, inc=1, device_id=dev, device_id_type=MESH)

    srcs = (u_hbm, f_hbm, w_hbm)
    cblocks = width // LANES

    def fetch(k):
        dep = halo if k < 2 else half

        def part(n, first, count):
            return [pltpu.make_async_copy(
                srcs[k].at[pl.ds(first, count), pl.ds(cb * LANES, LANES)],
                nat.at[k, cb, pl.ds(halo + first, count), :], loc_sem.at[k, cb, n]) for cb in range(cblocks)]
        return part(0, 0, dep) + part(1, rows - dep, dep), part(2, dep, rows - 2 * dep)

    local = [fetch(k) for k in range(3)]
    for copy in local[0][0] + local[0][1]:
        copy.start()
    params = [pltpu.make_async_copy(wts_hbm, wts_ref, par_sem.at[0]),
              pltpu.make_async_copy(gains_hbm, gains_ref, par_sem.at[1])]
    for copy in params:
        copy.start()
    for k in (1, 2):
        for copy in local[k][0] + local[k][1]:
            copy.start()
    pl.semaphore_wait(barrier, 4)

    def row_copies(k):
        dep = halo if k < 2 else half
        strip = lambda first: nat.at[k, :, pl.ds(first, dep), :]
        return [
            pltpu.make_async_remote_copy(strip(halo), strip(halo + rows), row_send.at[k, 0], row_recv.at[k, 0],
                                         device_id=above, device_id_type=MESH),
            pltpu.make_async_remote_copy(strip(halo + rows - dep), strip(halo - dep), row_send.at[k, 1],
                                         row_recv.at[k, 1], device_id=below, device_id_type=MESH),
        ]

    def col_copies(ref, dep, send, recv):
        return [
            pltpu.make_async_remote_copy(ref.at[:, pl.ds(org, dep), :], ref.at[:, pl.ds(org + width, dep), :],
                                         send.at[0], recv.at[0], device_id=left, device_id_type=MESH),
            pltpu.make_async_remote_copy(ref.at[:, pl.ds(org + width - dep, dep), :], ref.at[:, pl.ds(org - dep, dep), :],
                                         send.at[1], recv.at[1], device_id=right, device_id_type=MESH),
        ]

    rcopies = [row_copies(k) for k in range(3)]
    for k in range(3):
        for copy in local[k][0]:
            copy.wait()
        for copy in rcopies[k]:
            copy.start()
    for copy in params:
        copy.wait()

    def arrive(k, dst, factor):
        for copy in local[k][1] + rcopies[k]:
            copy.wait()
        for cb in range(cblocks):
            for b in range(nb):
                val = jnp.transpose(nat[k, cb, pl.ds(b, LANES, stride=nb), :])
                if factor is not None:
                    val = val * factor
                dst[b, pl.ds(org + cb * LANES, LANES), :] = val

    def depart(src, k, out, factor):
        for cb in range(cblocks):
            for b in range(nb):
                val = jnp.transpose(src[b, pl.ds(org + cb * LANES, LANES), :])
                if factor is not None:
                    val = val * factor
                nat[k, cb, pl.ds(b, LANES, stride=nb), :] = val
            out[:, pl.ds(cb * LANES, LANES)] = nat[k, cb, pl.ds(halo, rows), :]

    arrive(0, ubase.at[0], scale)
    for copy in col_copies(ubase.at[0], fdep, u_send.at[0], u_recv.at[0]):
        copy.start()
    wts = [[wts_ref[i, j] for j in range(3)] for i in range(3)]
    flip = [[wts_ref[2 - i, 2 - j] * (1.0 / 3.0) for j in range(3)] for i in range(3)]
    mid_wt = wts_ref[1, 1] + DT

    def sweep(body, base, count):
        for off in range(0, count, 8 * UNROLL):
            body(base + off, min(8 * UNROLL, count - off))

    def cover(step_body, dep, ahead):
        mark = width // 4 + 1

        def early():
            sweep(functools.partial(step_body, 1), org + mark, ahead)

        def first():
            sweep(functools.partial(step_body, 1), org + 1, mark - 1)
            sweep(functools.partial(step_body, 1), org + mark + ahead, width - 1 - mark - ahead)

        def middle():
            for j in range(2, PHASE + 1):
                sweep(functools.partial(step_body, j), org + j, width - 2 * j)

        def sides():
            for j in range(1, PHASE):
                sweep(functools.partial(step_body, j), org + j - dep, dep)
                sweep(functools.partial(step_body, j), org + width - j, dep)
            sweep(functools.partial(step_body, PHASE), org, PHASE)
            sweep(functools.partial(step_body, PHASE), org + width - PHASE, PHASE)
        return early, first, middle, sides

    def level(base, par, j):
        if j == 0:
            return base.at[par * BANKED]
        return base.at[(1 - par) * BANKED] if j == PHASE else inner.at[j - 1]

    def reaction(val, t, b, at):
        weight = mid_wt - val * val
        coef[t, b, at, :] = weight
        return weight

    def fwd_body(phase, forced, j, base, cols):
        par = phase % 2 if isinstance(phase, int) else lax.rem(phase, 2)
        src, dst, t = level(ubase, par, j - 1), level(ubase, par, j), phase * PHASE + (j - 1)
        at = pl.ds(base, cols)
        sums = stencil_blocks(lambda b, d: src[b, pl.ds(base + d, cols), :], wts,
                              lambda b, mid: reaction(mid, t, b, at), nb)
        for b in range(nb):
            dst[b, at, :] = sums[b] + gains_ref[t] * force[b, at, :] if forced else sums[b]

    sweep(functools.partial(fwd_body, 0, False, 1), org + 1, width - 2)
    arrive(1, force, scale)
    fcopies = col_copies(force, fdep, f_send, f_recv)
    for copy in fcopies:
        copy.start()

    for b in range(nb):
        at = pl.ds(org + 1, width - 2)
        inner[0, b, at, :] = inner[0, b, at, :] + gains_ref[0] * force[b, at, :]

    def adj_body(phase, j, base, cols):
        par = phase % 2 if isinstance(phase, int) else lax.rem(phase, 2)
        src, dst, t = level(lbase, par, j - 1), level(lbase, par, j), steps - (phase * PHASE + j)
        gain = gains_ref[t] * 3.0 ** (j - 1)
        at = pl.ds(base, cols)

        def centre(b, mid):
            if isinstance(phase, int) and phase == 0 and j == 1:
                acc[b, at, :] = gain * mid
            else:
                acc[b, at, :] += gain * mid
            return coef[t, b, at, :] - mid_wt * (2.0 / 3.0)
        sums = stencil_blocks(lambda b, d: src[b, pl.ds(base + d, cols), :], flip, centre, nb)
        for b in range(nb):
            dst[b, at, :] = sums[b] * 3.0 ** PHASE if j == PHASE else sums[b]

    def adj_sweeps(phase):
        return cover(functools.partial(adj_body, phase), adep, width * 5 // 8)

    def l_strips(phase):
        par = phase % 2 if isinstance(phase, int) else lax.rem(phase, 2)
        return col_copies(lbase.at[par * BANKED], adep, l_send.at[par], l_recv.at[par])

    def adj_turn(phase, _):
        for copy in l_strips(phase):
            copy.wait()
        early, first, middle, _ = adj_sweeps(phase + 1)
        early()
        adj_sweeps(phase)[3]()
        for copy in l_strips(phase + 1):
            copy.start()
        first()
        middle()
        return 0

    def fwd_sweeps(phase):
        return cover(functools.partial(fwd_body, phase, True), fdep, width // 4)

    def u_strips(phase):
        par = phase % 2 if isinstance(phase, int) else lax.rem(phase, 2)
        return col_copies(ubase.at[par * BANKED], fdep, u_send.at[par], u_recv.at[par])

    def fwd_close(phase):
        fwd_sweeps(phase)[3]()
        last = phase * PHASE + (PHASE - 1)
        for at in (pl.ds(org - PHASE, PHASE), pl.ds(org + width, PHASE)):
            for b in range(nb):
                reaction(inner[PHASE - 2, b, at, :], last, b, at)

    def fwd_turn(phase, _):
        for copy in u_strips(phase):
            copy.wait()

        @pl.when(phase == 0)
        def _():
            for copy in fcopies:
                copy.wait()
        early, first, middle, _ = fwd_sweeps(phase + 1)
        early()
        fwd_close(phase)
        for copy in u_strips(phase + 1):
            copy.start()
        first()
        middle()
        return 0

    fwd_sweeps(0)[2]()
    lax.fori_loop(0, phases - 1, fwd_turn, 0)

    arrive(2, lbase.at[0], None)
    for copy in l_strips(0):
        copy.start()
    for at in (pl.ds(0, org + 8), pl.ds(org + width - 8, org + 8)):
        acc[:, at, :] = jnp.zeros((nb, org + 8, LANES), jnp.float32)
    for copy in u_strips(phases - 1):
        copy.wait()
    early, first, middle, _ = adj_sweeps(0)
    early()
    fwd_close(phases - 1)
    first()
    middle()
    lax.fori_loop(0, phases - 1, adj_turn, 0)
    inside = width - 2 * PHASE
    lo_ref[:, pl.ds(PHASE, inside), :] = lbase[phases % 2 * BANKED, :, pl.ds(org + PHASE, inside), :]
    for copy in l_strips(phases - 1):
        copy.wait()
    depart(ubase.at[phases % 2 * BANKED], 0, uo_ref, 1.0 / scale)
    adj_sweeps(phases - 1)[3]()
    for edge in (0, width - PHASE):
        lo_ref[:, pl.ds(edge, PHASE), :] = lbase[phases % 2 * BANKED, :, pl.ds(org + edge, PHASE), :]


def unlane(tiles, org, u_ref, l_ref, a_ref, uo_hbm, go_hbm, gf_hbm, nat, sem):
    rows, width = tiles
    nb = l_ref.shape[0]
    halo = (nb * LANES - rows) // 2
    copies = [pltpu.make_async_copy(u_ref, uo_hbm, sem.at[0, 0])]
    copies[0].start()
    for k, (src, first, out) in enumerate(((l_ref, 0, go_hbm), (a_ref, org, gf_hbm))):
        for cb in range(width // LANES):
            for b in range(nb):
                nat[k, cb, pl.ds(b, LANES, stride=nb), :] = jnp.transpose(src[b, pl.ds(first + cb * LANES, LANES), :])
            copies.append(pltpu.make_async_copy(nat.at[k, cb, pl.ds(halo, rows), :],
                                                out.at[:, pl.ds(cb * LANES, LANES)], sem.at[k + 1, cb]))
            copies[-1].start()
    for copy in copies:
        copy.wait()


def solution(mesh):
    row_size, col_size, core_size = mesh.shape["row"], mesh.shape["col"], mesh.shape["core"]
    field_spec = P(("mem", "row"), ("col", "core"))

    def local_run(u_init, forcing, loss_weight, weights, gains):
        rows, width = u_init.shape
        steps = gains.shape[0]
        nb = -(-(rows + 4 * steps) // LANES)
        cols = width + 4 * PHASE + 8
        cblocks = width // LANES
        f32 = jnp.float32
        field = (nb, cols, LANES)
        dma = pltpu.SemaphoreType.DMA
        hbm, vmem = pl.BlockSpec(memory_space=pl.ANY), pl.BlockSpec(memory_space=pltpu.VMEM)
        lanes_out = pl.pallas_call(
            functools.partial(kernel, row_size, col_size, core_size, (rows, width, steps)),
            out_shape=[jax.ShapeDtypeStruct(dims, f32) for dims in ((rows, width), (nb, width, LANES), field)],
            in_specs=[hbm] * 5,
            out_specs=[vmem, vmem, vmem],
            scratch_shapes=[
                pltpu.SMEM(weights.shape, f32),
                pltpu.SMEM(gains.shape, f32),
                pltpu.VMEM((3, cblocks, nb * LANES, LANES), f32),
                pltpu.VMEM((2 * BANKED,) + field, f32),
                pltpu.VMEM((2 * BANKED,) + field, f32),
                pltpu.VMEM((PHASE,) + field, f32),
                pltpu.VMEM((steps,) + field, f32),
                pltpu.VMEM((BANKED,) + field, f32),
                dma((2,)),
                dma((3, cblocks, 3)),
                dma((3, 2)),
                dma((3, 2)),
                dma((2,)),
                dma((2,)),
                dma((2, 2)),
                dma((2, 2)),
                dma((2, 2)),
                dma((2, 2)),
            ],
            compiler_params=pltpu.CompilerParams(
                collective_id=0, has_side_effects=True, vmem_limit_bytes=52 * 1024 * 1024),
            name="steps",
        )(*(pltpu.with_memory_space_constraint(x, pltpu.HBM) for x in (weights, gains, u_init, forcing, loss_weight)))
        return pl.pallas_call(
            functools.partial(unlane, (rows, width), 2 * PHASE),
            out_shape=[jax.ShapeDtypeStruct((rows, width), f32)] * 3,
            in_specs=[vmem] * 3,
            out_specs=[hbm] * 3,
            scratch_shapes=[pltpu.VMEM((2, cblocks, nb * LANES, LANES), f32), dma((3, 2))],
            compiler_params=pltpu.CompilerParams(vmem_limit_bytes=16 * 1024 * 1024),
            name="unlane",
        )(*(pltpu.with_memory_space_constraint(x, pltpu.VMEM) for x in lanes_out))

    return jax.shard_map(local_run, mesh=mesh, in_specs=(field_spec, field_spec, field_spec, P(), P()),
                         out_specs=(field_spec, field_spec, field_spec), check_vma=False)
```

```python
import functools

import jax
import jax.numpy as jnp
from jax import lax
from jax.experimental import pallas as pl
from jax.experimental.pallas import tpu as pltpu
from jax.sharding import PartitionSpec as P


DT = 0.01
LANES = 128
PHASE = 8
BANKED = 4
UNROLL = 32
MESH = pl.DeviceIdType.MESH


def stencil_blocks(load, wts, centre, nb):
    part = {}
    for b in range(nb):
        left, mid, right = load(b, -1), load(b, 0), load(b, 1)
        part[b, -1] = (wts[0][0] * left + wts[0][1] * mid) + wts[0][2] * right
        part[b, 0] = (wts[1][0] * left + centre(b, mid) * mid) + wts[1][2] * right
        part[b, 1] = (wts[2][0] * left + wts[2][1] * mid) + wts[2][2] * right
    part[-1, -1] = pltpu.roll(part[nb - 1, -1], 1, 1)
    part[nb, 1] = pltpu.roll(part[0, 1], LANES - 1, 1)
    return [(part[b - 1, -1] + part[b, 0]) + part[b + 1, 1] for b in range(nb)]


def kernel(row_size, col_size, core_size, tiles, wts_hbm, gains_hbm, u_hbm, f_hbm, w_hbm, uo_ref, lo_ref, ao_ref,
           wts_ref, gains_ref, nat, ubase, lbase, inner, coef, forces, par_sem, loc_sem, row_send, row_recv, f_send, f_recv,
           u_send, u_recv, l_send, l_recv):
    rows, width, steps = tiles
    force, acc = forces.at[0], ao_ref
    nb = force.shape[0]
    halo = (nb * LANES - rows) // 2
    half = halo // 2
    fdep, adep = 2 * PHASE, PHASE
    org = fdep
    phases = steps // PHASE
    groups = width // 8
    scale = DT ** 0.5

    row_id, col_id, core_id = lax.axis_index("row"), lax.axis_index("col"), lax.axis_index("core")
    up, down = lax.rem(row_id + row_size - 1, row_size), lax.rem(row_id + 1, row_size)
    flat = col_id * core_size + core_id
    total = col_size * core_size
    lflat, rflat = lax.rem(flat + total - 1, total), lax.rem(flat + 1, total)
    above, below = {"row": up}, {"row": down}
    left = {"col": lax.div(lflat, core_size), "core": lax.rem(lflat, core_size)}
    right = {"col": lax.div(rflat, core_size), "core": lax.rem(rflat, core_size)}

    barrier = pltpu.get_barrier_semaphore()
    for dev in (above, below, left, right):
        pl.semaphore_signal(barrier, inc=1, device_id=dev, device_id_type=MESH)

    srcs = (u_hbm, f_hbm, w_hbm)
    cblocks = width // LANES

    def fetch(k):
        dep = halo if k < 2 else half

        def part(n, first, count):
            return [pltpu.make_async_copy(
                srcs[k].at[pl.ds(first, count), pl.ds(cb * LANES, LANES)],
                nat.at[k, cb, pl.ds(halo + first, count), :], loc_sem.at[k, cb, n]) for cb in range(cblocks)]
        return part(0, 0, dep) + part(1, rows - dep, dep), part(2, dep, rows - 2 * dep)

    local = [fetch(k) for k in range(3)]
    for copy in local[0][0] + local[0][1]:
        copy.start()
    params = [pltpu.make_async_copy(wts_hbm, wts_ref, par_sem.at[0]),
              pltpu.make_async_copy(gains_hbm, gains_ref, par_sem.at[1])]
    for copy in params:
        copy.start()
    for k in (1, 2):
        for copy in local[k][0] + local[k][1]:
            copy.start()
    pl.semaphore_wait(barrier, 4)

    def row_copies(k):
        dep = halo if k < 2 else half
        strip = lambda first: nat.at[k, :, pl.ds(first, dep), :]
        return [
            pltpu.make_async_remote_copy(strip(halo), strip(halo + rows), row_send.at[k, 0], row_recv.at[k, 0],
                                         device_id=above, device_id_type=MESH),
            pltpu.make_async_remote_copy(strip(halo + rows - dep), strip(halo - dep), row_send.at[k, 1],
                                         row_recv.at[k, 1], device_id=below, device_id_type=MESH),
        ]

    def col_copies(ref, dep, send, recv):
        return [
            pltpu.make_async_remote_copy(ref.at[:, pl.ds(org, dep), :], ref.at[:, pl.ds(org + width, dep), :],
                                         send.at[0], recv.at[0], device_id=left, device_id_type=MESH),
            pltpu.make_async_remote_copy(ref.at[:, pl.ds(org + width - dep, dep), :], ref.at[:, pl.ds(org - dep, dep), :],
                                         send.at[1], recv.at[1], device_id=right, device_id_type=MESH),
        ]

    rcopies = [row_copies(k) for k in range(3)]
    for k in range(3):
        for copy in local[k][0]:
            copy.wait()
        for copy in rcopies[k]:
            copy.start()
    for copy in params:
        copy.wait()

    def arrive(k, dst, factor):
        for copy in local[k][1] + rcopies[k]:
            copy.wait()
        for cb in range(cblocks):
            for b in range(nb):
                val = jnp.transpose(nat[k, cb, pl.ds(b, LANES, stride=nb), :])
                if factor is not None:
                    val = val * factor
                dst[b, pl.ds(org + cb * LANES, LANES), :] = val

    def depart(src, k, out, factor):
        for cb in range(cblocks):
            for b in range(nb):
                val = jnp.transpose(src[b, pl.ds(org + cb * LANES, LANES), :])
                if factor is not None:
                    val = val * factor
                nat[k, cb, pl.ds(b, LANES, stride=nb), :] = val
            out[:, pl.ds(cb * LANES, LANES)] = nat[k, cb, pl.ds(halo, rows), :]

    arrive(0, ubase.at[0], scale)
    for copy in col_copies(ubase.at[0], fdep, u_send.at[0], u_recv.at[0]):
        copy.start()
    wts = [[wts_ref[i, j] for j in range(3)] for i in range(3)]
    flip = [[wts_ref[2 - i, 2 - j] * (1.0 / 3.0) for j in range(3)] for i in range(3)]
    mid_wt = wts_ref[1, 1] + DT

    def sweep(body, base, count):
        for off in range(0, count, 8 * UNROLL):
            body(base + off, min(8 * UNROLL, count - off))

    def cover(step_body, dep, ahead):
        mark = width // 4 + 1

        def early():
            sweep(functools.partial(step_body, 1), org + mark, ahead)

        def first():
            sweep(functools.partial(step_body, 1), org + 1, mark - 1)
            sweep(functools.partial(step_body, 1), org + mark + ahead, width - 1 - mark - ahead)

        def middle():
            for j in range(2, PHASE + 1):
                sweep(functools.partial(step_body, j), org + j, width - 2 * j)

        def sides():
            for j in range(1, PHASE):
                sweep(functools.partial(step_body, j), org + j - dep, dep)
                sweep(functools.partial(step_body, j), org + width - j, dep)
            sweep(functools.partial(step_body, PHASE), org, PHASE)
            sweep(functools.partial(step_body, PHASE), org + width - PHASE, PHASE)
        return early, first, middle, sides

    def level(base, par, j):
        if j == 0:
            return base.at[par * BANKED]
        return base.at[(1 - par) * BANKED] if j == PHASE else inner.at[j - 1]

    def reaction(val, t, b, at):
        weight = mid_wt - val * val
        coef[t, b, at, :] = weight
        return weight

    def fwd_body(phase, forced, j, base, cols):
        par = phase % 2 if isinstance(phase, int) else lax.rem(phase, 2)
        src, dst, t = level(ubase, par, j - 1), level(ubase, par, j), phase * PHASE + (j - 1)
        at = pl.ds(base, cols)
        sums = stencil_blocks(lambda b, d: src[b, pl.ds(base + d, cols), :], wts,
                              lambda b, mid: reaction(mid, t, b, at), nb)
        for b in range(nb):
            dst[b, at, :] = sums[b] + gains_ref[t] * force[b, at, :] if forced else sums[b]

    sweep(functools.partial(fwd_body, 0, False, 1), org + 1, width - 2)
    arrive(1, force, scale)
    fcopies = col_copies(force, fdep, f_send, f_recv)
    for copy in fcopies:
        copy.start()

    for b in range(nb):
        at = pl.ds(org + 1, width - 2)
        inner[0, b, at, :] = inner[0, b, at, :] + gains_ref[0] * force[b, at, :]

    def adj_body(phase, j, base, cols):
        par = phase % 2 if isinstance(phase, int) else lax.rem(phase, 2)
        src, dst, t = level(lbase, par, j - 1), level(lbase, par, j), steps - (phase * PHASE + j)
        gain = gains_ref[t] * 3.0 ** (j - 1)
        at = pl.ds(base, cols)

        def centre(b, mid):
            if isinstance(phase, int) and phase == 0 and j == 1:
                acc[b, at, :] = gain * mid
            else:
                acc[b, at, :] += gain * mid
            return coef[t, b, at, :] - mid_wt * (2.0 / 3.0)
        sums = stencil_blocks(lambda b, d: src[b, pl.ds(base + d, cols), :], flip, centre, nb)
        for b in range(nb):
            dst[b, at, :] = sums[b] * 3.0 ** PHASE if j == PHASE else sums[b]

    def adj_sweeps(phase):
        return cover(functools.partial(adj_body, phase), adep, width * 11 // 16)

    def l_strips(phase):
        par = phase % 2 if isinstance(phase, int) else lax.rem(phase, 2)
        return col_copies(lbase.at[par * BANKED], adep, l_send.at[par], l_recv.at[par])

    def adj_turn(phase, _):
        for copy in l_strips(phase):
            copy.wait()
        early, first, middle, _ = adj_sweeps(phase + 1)
        early()
        adj_sweeps(phase)[3]()
        for copy in l_strips(phase + 1):
            copy.start()
        first()
        middle()
        return 0

    def fwd_sweeps(phase):
        return cover(functools.partial(fwd_body, phase, True), fdep, width * 3 // 8)

    def u_strips(phase):
        par = phase % 2 if isinstance(phase, int) else lax.rem(phase, 2)
        return col_copies(ubase.at[par * BANKED], fdep, u_send.at[par], u_recv.at[par])

    def fwd_close(phase):
        fwd_sweeps(phase)[3]()
        last = phase * PHASE + (PHASE - 1)
        for at in (pl.ds(org - PHASE, PHASE), pl.ds(org + width, PHASE)):
            for b in range(nb):
                reaction(inner[PHASE - 2, b, at, :], last, b, at)

    def fwd_turn(phase, _):
        for copy in u_strips(phase):
            copy.wait()

        @pl.when(phase == 0)
        def _():
            for copy in fcopies:
                copy.wait()
        early, first, middle, _ = fwd_sweeps(phase + 1)
        early()
        fwd_close(phase)
        for copy in u_strips(phase + 1):
            copy.start()
        first()
        middle()
        return 0

    fwd_sweeps(0)[2]()
    lax.fori_loop(0, phases - 1, fwd_turn, 0)

    arrive(2, lbase.at[0], None)
    for copy in l_strips(0):
        copy.start()
    for at in (pl.ds(0, org + 8), pl.ds(org + width - 8, org + 8)):
        acc[:, at, :] = jnp.zeros((nb, org + 8, LANES), jnp.float32)
    for copy in u_strips(phases - 1):
        copy.wait()
    early, first, middle, _ = adj_sweeps(0)
    early()
    fwd_close(phases - 1)
    first()
    middle()
    lax.fori_loop(0, phases - 1, adj_turn, 0)
    inside = width - 2 * PHASE
    lo_ref[:, pl.ds(PHASE, inside), :] = lbase[phases % 2 * BANKED, :, pl.ds(org + PHASE, inside), :]
    for copy in l_strips(phases - 1):
        copy.wait()
    depart(ubase.at[phases % 2 * BANKED], 0, uo_ref, 1.0 / scale)
    adj_sweeps(phases - 1)[3]()
    for edge in (0, width - PHASE):
        lo_ref[:, pl.ds(edge, PHASE), :] = lbase[phases % 2 * BANKED, :, pl.ds(org + edge, PHASE), :]


def unlane(tiles, org, u_ref, l_ref, a_ref, uo_hbm, go_hbm, gf_hbm, nat, sem):
    rows, width = tiles
    nb = l_ref.shape[0]
    halo = (nb * LANES - rows) // 2
    copies = [pltpu.make_async_copy(u_ref, uo_hbm, sem.at[0, 0])]
    copies[0].start()
    for k, (src, first, out) in enumerate(((l_ref, 0, go_hbm), (a_ref, org, gf_hbm))):
        for cb in range(width // LANES):
            for b in range(nb):
                nat[k, cb, pl.ds(b, LANES, stride=nb), :] = jnp.transpose(src[b, pl.ds(first + cb * LANES, LANES), :])
            copies.append(pltpu.make_async_copy(nat.at[k, cb, pl.ds(halo, rows), :],
                                                out.at[:, pl.ds(cb * LANES, LANES)], sem.at[k + 1, cb]))
            copies[-1].start()
    for copy in copies:
        copy.wait()


def solution(mesh):
    row_size, col_size, core_size = mesh.shape["row"], mesh.shape["col"], mesh.shape["core"]
    field_spec = P(("mem", "row"), ("col", "core"))

    def local_run(u_init, forcing, loss_weight, weights, gains):
        rows, width = u_init.shape
        steps = gains.shape[0]
        nb = -(-(rows + 4 * steps) // LANES)
        cols = width + 4 * PHASE + 8
        cblocks = width // LANES
        f32 = jnp.float32
        field = (nb, cols, LANES)
        dma = pltpu.SemaphoreType.DMA
        hbm, vmem = pl.BlockSpec(memory_space=pl.ANY), pl.BlockSpec(memory_space=pltpu.VMEM)
        lanes_out = pl.pallas_call(
            functools.partial(kernel, row_size, col_size, core_size, (rows, width, steps)),
            out_shape=[jax.ShapeDtypeStruct(dims, f32) for dims in ((rows, width), (nb, width, LANES), field)],
            in_specs=[hbm] * 5,
            out_specs=[vmem, vmem, vmem],
            scratch_shapes=[
                pltpu.SMEM(weights.shape, f32),
                pltpu.SMEM(gains.shape, f32),
                pltpu.VMEM((3, cblocks, nb * LANES, LANES), f32),
                pltpu.VMEM((2 * BANKED,) + field, f32),
                pltpu.VMEM((2 * BANKED,) + field, f32),
                pltpu.VMEM((PHASE,) + field, f32),
                pltpu.VMEM((steps,) + field, f32),
                pltpu.VMEM((BANKED,) + field, f32),
                dma((2,)),
                dma((3, cblocks, 3)),
                dma((3, 2)),
                dma((3, 2)),
                dma((2,)),
                dma((2,)),
                dma((2, 2)),
                dma((2, 2)),
                dma((2, 2)),
                dma((2, 2)),
            ],
            compiler_params=pltpu.CompilerParams(
                collective_id=0, has_side_effects=True, vmem_limit_bytes=52 * 1024 * 1024),
            name="steps",
        )(*(pltpu.with_memory_space_constraint(x, pltpu.HBM) for x in (weights, gains, u_init, forcing, loss_weight)))
        return pl.pallas_call(
            functools.partial(unlane, (rows, width), 2 * PHASE),
            out_shape=[jax.ShapeDtypeStruct((rows, width), f32)] * 3,
            in_specs=[vmem] * 3,
            out_specs=[hbm] * 3,
            scratch_shapes=[pltpu.VMEM((2, cblocks, nb * LANES, LANES), f32), dma((3, 2))],
            compiler_params=pltpu.CompilerParams(vmem_limit_bytes=16 * 1024 * 1024),
            name="unlane",
        )(*(pltpu.with_memory_space_constraint(x, pltpu.VMEM) for x in lanes_out))

    return jax.shard_map(local_run, mesh=mesh, in_specs=(field_spec, field_spec, field_spec, P(), P()),
                         out_specs=(field_spec, field_spec, field_spec), check_vma=False)
```
